512 devices in a mesh: grp: 16 (over z), cand: 32 (over y, x, core).
Axes of the slice: x: 4, y: 4, z: 16, core: 2. Of those that a mesh axis runs over, the one named last changes fastest.
Arguments:
- embeddings: bfloat16 [384, 1024, 1024], P('grp', 'cand'), may hold values from -6 to 6
- hidden_weight: bfloat16 [2048, 1024], P('cand'), may hold values from -0.1875 to 0.1875
- score_weight: bfloat16 [2048], replicated, may hold values from -0.5 to 0.5
- relevance: int32 [384, 1024], P('grp', 'cand'), may hold values from 0 to 4
- rank_pos: int32 [384, 1024], P('grp', 'cand'), may hold values from 0 to 1023, as said below
- ideal_dcg: float32 [384], P('grp'), may hold values from 32 to 128
Outputs:
- grad_hidden: float32 [2048, 1024], P('cand')
- lambdas: float32 [384, 1024], P('grp', 'cand')
The draws below stay inside these ranges and needn't reach their ends.
Inputs may be any that keep to these rules, and one draw needn't show every extreme that they name: `rank_pos`: in each group the rank positions are a permutation of 0 to 1023.
All inputs are finite; a program needn't handle non-finite values.
Results may differ from the reference program's by a relative error of at most 0.006.
Values may be sent and summed in bfloat16 or wider, within the bound.
No kernel may reach another device: no remote copies, remote signals or barrier semaphores. Data moves between devices by JAX's collectives and lax.ppermute only.
A program may use at most 64 MiB of HBM per device.

```python
import math
import jax
import jax.numpy as jnp
from jax import lax

EMBED = 1024
HIDDEN_SIZE = 2048
CANDS = 1024
GRP_DEV = 24
GROUPS = 384
N_GRP = 16
N_CAND = 32


def draw_rank_pos(key, part):
    jitter = jax.random.randint(jax.random.fold_in(key, 11), (GROUPS, CANDS), 0, CANDS // 4)
    order_key = jnp.arange(CANDS, dtype=jnp.int32)[None, :] * 4 + jitter
    order = jnp.argsort(order_key, axis=1, stable=True)
    return jnp.argsort(order, axis=1, stable=True).astype(jnp.int32)


def place_ends(array, rng, smallest, high):
    longest = array.shape.index(max(array.shape))
    spots = []
    for shift in (0, 1):
        where = [jax.random.randint(jax.random.fold_in(rng, axis), (), 0, length) for axis, length in enumerate(array.shape)]
        where[longest] = (where[longest] + shift) % array.shape[longest]
        spots.append(tuple(where))
    return array.at[spots[0]].set(smallest).at[spots[1]].set(high)


def block_scale(rng, dims, cuts, least, top_value):
    def one(axis_at, blocks):
        steps = jax.random.uniform(jax.random.fold_in(jax.random.fold_in(rng, 6), axis_at), (blocks,), jnp.float32, least / len(cuts), top_value / len(cuts))
        return jnp.repeat(jnp.exp(steps), dims[axis_at] // blocks).reshape((-1,) + (1,) * (len(dims) - axis_at - 1))

    gain = one(*cuts[0])
    for cut in cuts[1:]:
        gain = gain * one(*cut)
    return gain


def normal_values(key, dims, spread, most, shards=(), held_as=jnp.bfloat16):
    array = spread * jax.random.normal(key, dims, jnp.float32)
    if shards:
        array = array * block_scale(key, dims, shards, -0.22, 0.18)
    return jnp.clip(array, -most, most).astype(held_as)


def setup_inputs(seed: int = 0) -> dict:
    key_of = jax.random.split(jax.random.key(seed), 7)
    embeddings = normal_values(key_of[0], (GROUPS, CANDS, EMBED), 1.0, 6.0, ((0, 16), (1, 32)))
    hidden_weight = normal_values(key_of[1], (HIDDEN_SIZE, EMBED), EMBED ** -0.5, 0.1875, ((0, 32),))
    score_weight = normal_values(key_of[2], (HIDDEN_SIZE,), (HIDDEN_SIZE // 16) ** -0.5, 0.5)
    relevance = place_ends(jax.random.randint(key_of[3], (GROUPS, CANDS), 0, 5), jax.random.fold_in(key_of[3], 1), 0, 4).astype(jnp.int32)
    rank_pos = draw_rank_pos(jax.random.fold_in(key_of[6], 71), 0)
    ideal_dcg = jnp.clip(jnp.exp(math.log(128.0) - 1.3862944 * jax.random.uniform(key_of[5], (GROUPS,), jnp.float32) ** block_scale(key_of[5], (GROUPS,), ((0, 16),), -0.2, 0.2)), 32.0, 128.0)
    return dict(embeddings=embeddings, hidden_weight=hidden_weight, score_weight=score_weight, relevance=relevance, rank_pos=rank_pos, ideal_dcg=ideal_dcg)


EPS = 1e-06

def pair_lambdas(own_score, own_gain, own_disc, far_score, far_gain, far_disc, ideal):
    gain_diff = far_gain[..., None, :] - own_gain[..., :, None]
    toward = jnp.sign(gain_diff)
    weight = jnp.abs(gain_diff) * jnp.abs(far_disc[..., None, :] - own_disc[..., :, None]) / ideal[..., None, None]
    margin = own_score[..., :, None] - far_score[..., None, :]
    return lax.optimization_barrier(jnp.sum(weight * toward * jax.nn.sigmoid(toward * margin), axis=-1))

def reference(embeddings, hidden_weight, score_weight, relevance, rank_pos, ideal_dcg):

    def group_scores(cand_rows):
        pre_act = jnp.dot(cand_rows, hidden_weight.T, preferred_element_type=jnp.float32)
        acts = jax.nn.gelu(pre_act).astype(jnp.bfloat16)
        return jnp.dot(acts, score_weight, preferred_element_type=jnp.float32)
    scores = lax.map(group_scores, embeddings)
    gain_vals = jnp.exp2(relevance.astype(jnp.float32)) - 1.0
    discount = 1.0 / jnp.log2(2.0 + rank_pos.astype(jnp.float32))

    def group_lambdas(packed):
        own_score, own_gain, own_disc, ideal = packed
        return pair_lambdas(own_score, own_gain, own_disc, own_score, own_gain, own_disc, ideal)
    lambdas = lax.map(group_lambdas, (scores, gain_vals, discount, ideal_dcg))
    local = CANDS // N_CAND
    weight_row = score_weight.astype(jnp.float32)
    zero_index = jnp.zeros((), jnp.int32)

    def add_block(running, index):
        first = (index // N_CAND * GRP_DEV).astype(jnp.int32)
        cand_first = (index % N_CAND * local).astype(jnp.int32)
        block = lax.dynamic_slice(embeddings, (first, cand_first, zero_index), (GRP_DEV, local, EMBED))
        cand_rows = block.reshape(GRP_DEV * local, EMBED)
        block_lam = lax.dynamic_slice(lambdas, (first, cand_first), (GRP_DEV, local)).reshape(GRP_DEV * local)
        pre_act = jnp.dot(cand_rows, hidden_weight.T, preferred_element_type=jnp.float32)
        _, pull = jax.vjp(jax.nn.gelu, pre_act)
        upstream = block_lam[:, None] * weight_row[None, :]
        grad_pre = pull(upstream)[0].astype(jnp.bfloat16)
        term = lax.dot_general(grad_pre, cand_rows, (((0,), (0,)), ((), ())), preferred_element_type=jnp.float32)
        rounded = lax.optimization_barrier(term.astype(jnp.bfloat16))
        return (running + rounded.astype(jnp.float32), None)
    total, _ = lax.scan(add_block, jnp.zeros((HIDDEN_SIZE, EMBED), jnp.float32), jnp.arange(N_GRP * N_CAND, dtype=jnp.int32))
    scale = lax.rsqrt(jnp.mean(total * total) + EPS)
    return (total * scale, lambdas)
```

```python
import jax
import jax.numpy as jnp
from jax import lax
from jax.sharding import Mesh
from jax.sharding import PartitionSpec as P

EPS = 1e-06
GELU_A = 0.7978845608028654
GELU_B = 0.044715
CHIPS = ("y", "x")
CAND = ("y", "x", "c")


def spread(value, axis, size):
    copies = jnp.broadcast_to(value[None], (size, *value.shape))
    return lax.all_to_all(copies, axis, split_axis=0, concat_axis=0, tiled=True)


def per_device(embeddings, hidden_weight, score_weight, relevance, rank_pos, ideal_dcg):
    groups, local, width = embeddings.shape
    owned_rows = hidden_weight.shape[0]
    cores = lax.axis_size("c")
    chips = lax.axis_size("y") * lax.axis_size("x")
    planes = lax.axis_size("z")
    core = lax.axis_index("c")
    chip = lax.axis_index("y") * lax.axis_size("x") + lax.axis_index("x")
    own = embeddings.reshape(groups * local, width)

    other = lax.ppermute(own, "c", [(0, 1), (1, 0)])
    labels = spread(jnp.stack([relevance, rank_pos]), CAND, chips * cores)
    weight = spread(hidden_weight, CHIPS, chips).reshape(chips * owned_rows, width)

    labels = labels.reshape(chips, cores, 2, groups, local).transpose(2, 3, 0, 1, 4)
    own_labels = lax.dynamic_index_in_dim(labels, chip, 2, keepdims=False)
    labels = labels.reshape(2, groups, chips * cores * local)
    own_labels = own_labels.reshape(2, groups, cores * local)
    gain = lambda v: jnp.exp2(v.astype(jnp.float32)) - 1.0
    disc = lambda v: 1.0 / jnp.log2(2.0 + v.astype(jnp.float32))
    gain_diff = gain(labels[0])[:, None, :] - gain(own_labels[0])[:, :, None]
    disc_diff = jnp.abs(disc(labels[1])[:, None, :] - disc(own_labels[1])[:, :, None])
    pull = gain_diff * disc_diff / ideal_dcg[:, None, None]

    both = jnp.concatenate([own, other], axis=0)
    unit_weight = lax.dynamic_index_in_dim(
        score_weight.reshape(chips, cores, owned_rows), core, 1, keepdims=False
    ).reshape(chips * owned_rows).astype(jnp.float32)
    pre = lax.dot_general(
        weight, both, (((1,), (1,)), ((), ())), preferred_element_type=jnp.float32
    )
    tanh = jnp.tanh(GELU_A * (pre + GELU_B * pre * pre * pre))
    acts = (0.5 * pre * (1.0 + tanh)).astype(jnp.bfloat16).astype(jnp.float32)
    slope = 0.5 * (1.0 + tanh) + 0.5 * pre * (1.0 - tanh * tanh) * (
        GELU_A * (1.0 + 3.0 * GELU_B * pre * pre)
    )
    part = jnp.sum(acts * unit_weight[:, None], axis=0).reshape(2, groups, local)
    part = jnp.where(core == 0, part, part[::-1])
    pair = lax.psum(part, "c")
    scores = spread(pair, CHIPS, chips)
    scores = scores.transpose(2, 0, 1, 3).reshape(groups, chips * cores * local)
    own_scores = pair.transpose(1, 0, 2).reshape(groups, cores * local)
    margin = own_scores[:, :, None] - scores[:, None, :]
    pair_lam = jnp.sum(
        pull * jax.nn.sigmoid(jnp.where(gain_diff < 0.0, -margin, margin)), axis=-1
    )
    pair_lam = pair_lam.reshape(groups, cores, local).transpose(1, 0, 2)
    pair_lam = jnp.where(core == 0, pair_lam, pair_lam[::-1])
    lambdas = pair_lam[0]

    upstream = pair_lam.reshape(-1)[None, :] * unit_weight[:, None]
    grad_pre = (upstream * slope).astype(jnp.bfloat16)
    term = lax.dot_general(
        grad_pre, both, (((1,), (0,)), ((), ())), preferred_element_type=jnp.float32
    ).astype(jnp.bfloat16)
    terms = lax.all_to_all(
        term.reshape(chips, owned_rows, width), CHIPS, split_axis=0, concat_axis=0, tiled=True
    )
    owned = jnp.sum(terms.astype(jnp.float32), axis=0)
    pieces = lax.all_to_all(
        owned.reshape(planes, owned_rows // planes, width), "z", split_axis=0, concat_axis=0, tiled=True
    )
    piece = jnp.sum(pieces, axis=0)
    total = spread(piece, "z", planes).reshape(owned_rows, width)
    squares = jnp.sum(spread(jnp.sum(total * total), CAND, chips * cores))
    entries = owned_rows * width * chips * cores
    return total * lax.rsqrt(squares / entries + EPS), lambdas


def solution(mesh):
    fine = Mesh(mesh.devices.reshape(mesh.devices.shape[0], 4, 4, 2), ("z", "y", "x", "c"))
    return jax.shard_map(
        per_device,
        mesh=fine,
        in_specs=(
            P("z", CAND, None),
            P(CAND, None),
            P(),
            P("z", CAND),
            P("z", CAND),
            P("z"),
        ),
        out_specs=(P(CAND, None), P("z", CAND)),
        check_vma=False,
    )
```

```python
import jax
import jax.numpy as jnp
from jax import lax
from jax.sharding import Mesh
from jax.sharding import PartitionSpec as P


EPS = 1e-06
GELU_A = 0.7978845608028654
GELU_B = 0.044715
CHIPS = ("y", "x")
CAND = ("y", "x", "c")


def spread(value, axis, size):
    copies = jnp.broadcast_to(value[None], (size, *value.shape))
    return lax.all_to_all(copies, axis, split_axis=0, concat_axis=0, tiled=True)


def per_device(embeddings, hidden_weight, score_weight, relevance, rank_pos, ideal_dcg):
    groups, local, width = embeddings.shape
    owned_rows = hidden_weight.shape[0]
    cores = lax.axis_size("c")
    chips = lax.axis_size("y") * lax.axis_size("x")
    planes = lax.axis_size("z")
    core = lax.axis_index("c")
    own = embeddings.reshape(groups * local, width)

    weight = spread(hidden_weight, CHIPS, chips).reshape(chips * owned_rows, width)
    other = lax.ppermute(own, "c", [(0, 1), (1, 0)])
    own_labels = lax.all_gather(jnp.stack([relevance, rank_pos]), "c")
    labels = lax.all_gather(lax.all_gather(own_labels, "x"), "y")
    own_labels = own_labels.transpose(1, 2, 0, 3).reshape(2, groups, cores * local)
    labels = labels.transpose(3, 4, 0, 1, 2, 5).reshape(2, groups, chips * cores * local)
    gain = lambda v: jnp.exp2(v.astype(jnp.float32)) - 1.0
    disc = lambda v: 1.0 / jnp.log2(2.0 + v.astype(jnp.float32))
    gain_diff = gain(labels[0])[:, None, :] - gain(own_labels[0])[:, :, None]
    disc_diff = jnp.abs(disc(labels[1])[:, None, :] - disc(own_labels[1])[:, :, None])
    pull = gain_diff * disc_diff / ideal_dcg[:, None, None]

    both = jnp.concatenate([own, other], axis=0)
    unit_weight = lax.dynamic_index_in_dim(
        score_weight.reshape(chips, cores, owned_rows), core, 1, keepdims=False
    ).reshape(chips * owned_rows).astype(jnp.float32)
    pre = lax.dot_general(
        weight, both, (((1,), (1,)), ((), ())), preferred_element_type=jnp.float32
    )
    tanh = jnp.tanh(GELU_A * (pre + GELU_B * pre * pre * pre))
    acts = (0.5 * pre * (1.0 + tanh)).astype(jnp.bfloat16).astype(jnp.float32)
    slope = 0.5 * (1.0 + tanh) + 0.5 * pre * (1.0 - tanh * tanh) * (
        GELU_A * (1.0 + 3.0 * GELU_B * pre * pre)
    )
    part = jnp.sum(acts * unit_weight[:, None], axis=0).reshape(2, groups, local)
    part = jnp.where(core == 0, part, part[::-1])
    pair = lax.psum(part, "c")
    scores = spread(pair, CHIPS, chips)
    scores = scores.transpose(2, 0, 1, 3).reshape(groups, chips * cores * local)
    own_scores = pair.transpose(1, 0, 2).reshape(groups, cores * local)
    margin = own_scores[:, :, None] - scores[:, None, :]
    pair_lam = jnp.sum(
        pull * jax.nn.sigmoid(jnp.where(gain_diff < 0.0, -margin, margin)), axis=-1
    )
    pair_lam = pair_lam.reshape(groups, cores, local).transpose(1, 0, 2)
    pair_lam = jnp.where(core == 0, pair_lam, pair_lam[::-1])
    lambdas = pair_lam[0]

    upstream = pair_lam.reshape(-1)[None, :] * unit_weight[:, None]
    grad_pre = (upstream * slope).astype(jnp.bfloat16)
    term = lax.dot_general(
        grad_pre, both, (((1,), (0,)), ((), ())), preferred_element_type=jnp.float32
    ).astype(jnp.bfloat16)
    terms = lax.all_to_all(
        term.reshape(chips, owned_rows, width), CHIPS, split_axis=0, concat_axis=0, tiled=True
    )
    owned = jnp.sum(terms.astype(jnp.float32), axis=0)
    pieces = lax.all_to_all(
        owned.astype(jnp.bfloat16).reshape(planes, owned_rows // planes, width), "z", split_axis=0, concat_axis=0, tiled=True
    )
    piece = jnp.sum(pieces.astype(jnp.float32), axis=0).astype(jnp.bfloat16)
    total = spread(piece, "z", planes).reshape(owned_rows, width).astype(jnp.float32)
    squares = jnp.sum(spread(jnp.sum(total * total), CAND, chips * cores))
    entries = owned_rows * width * chips * cores
    return total * lax.rsqrt(squares / entries + EPS), lambdas


def solution(mesh):
    fine = Mesh(mesh.devices.reshape(mesh.devices.shape[0], 4, 4, 2), ("z", "y", "x", "c"))
    return jax.shard_map(
        per_device,
        mesh=fine,
        in_specs=(
            P("z", CAND, None),
            P(CAND, None),
            P(),
            P("z", CAND),
            P("z", CAND),
            P("z"),
        ),
        out_specs=(P(CAND, None), P("z", CAND)),
        check_vma=False,
    )
```

```python
import jax
import jax.numpy as jnp
from jax import lax
from jax.experimental import pallas as pl
from jax.experimental.pallas import tpu as pltpu
from jax.sharding import Mesh
from jax.sharding import PartitionSpec as P

EPS = 1e-06
GELU_A = 0.7978845608028654
GELU_B = 0.044715
CHIPS = ("y", "x")
CAND = ("y", "x", "c")
MIB = 1 << 20
f32 = jnp.float32
bf16 = jnp.bfloat16


def spread(value, axis, size):
    copies = jnp.broadcast_to(value[None], (size, *value.shape))
    return lax.all_to_all(copies, axis, split_axis=0, concat_axis=0, tiled=True)


def score_kernel(weight_ref, own_ref, other_ref, unit_ref, pre_ref, part_ref):
    @pl.when(pl.program_id(0) == 0)
    def _():
        part_ref[...] = jnp.zeros_like(part_ref)

    weight = weight_ref[...]
    unit = unit_ref[...]
    cut = 256
    for half, rows_ref in enumerate((own_ref, other_ref)):
        count = rows_ref.shape[0]
        for first in range(0, count, cut):
            pre = lax.dot_general(
                weight,
                rows_ref[first : first + cut, :],
                (((1,), (1,)), ((), ())),
                preferred_element_type=f32,
            )
            cols = slice(half * count + first, half * count + first + cut)
            pre_ref[:, cols] = pre
            tanh = jnp.tanh(pre * (GELU_A + (GELU_A * GELU_B) * (pre * pre)))
            part = 0.5 * pre
            acts = (part + part * tanh).astype(bf16).astype(f32)
            part_ref[:, cols] += jnp.sum(acts * unit, axis=0, keepdims=True)


def score(weight, own, other, unit):
    units, width = weight.shape
    count = own.shape[0]
    block = units // 2
    return pl.pallas_call(
        score_kernel,
        grid=(units // block,),
        in_specs=[
            pl.BlockSpec((block, width), lambda i: (i, 0)),
            pl.BlockSpec((count, width), lambda i: (0, 0)),
            pl.BlockSpec((count, width), lambda i: (0, 0)),
            pl.BlockSpec((block, 1), lambda i: (i, 0)),
        ],
        out_specs=[
            pl.BlockSpec((block, 2 * count), lambda i: (i, 0)),
            pl.BlockSpec((1, 2 * count), lambda i: (0, 0)),
        ],
        out_shape=[
            pltpu.HBM((units, 2 * count), f32),
            jax.ShapeDtypeStruct((1, 2 * count), f32),
        ],
        compiler_params=pltpu.CompilerParams(vmem_limit_bytes=32 * MIB),
        cost_estimate=pl.CostEstimate(
            flops=4 * units * width * count,
            bytes_accessed=12 * MIB,
            transcendentals=2 * units * count,
        ),
        name="score",
    )(weight, own, other, unit)


def slope_kernel(pre_ref, unit_ref, slope_ref):
    pre = pre_ref[...]
    square = pre * pre
    tanh = jnp.tanh(pre * (GELU_A + (GELU_A * GELU_B) * square))
    slope_ref[...] = (0.5 * unit_ref[...]) * (
        (1.0 + tanh)
        + pre * (1.0 - tanh * tanh) * (GELU_A + (3.0 * GELU_A * GELU_B) * square)
    )


def slopes(pre, unit):
    units, count = pre.shape
    block = 128
    return pl.pallas_call(
        slope_kernel,
        grid=(units // block,),
        in_specs=[
            pl.BlockSpec((block, count), lambda i: (i, 0)),
            pl.BlockSpec((block, 1), lambda i: (i, 0)),
        ],
        out_specs=pl.BlockSpec((block, count), lambda i: (i, 0)),
        out_shape=pltpu.HBM((units, count), f32),
        compiler_params=pltpu.CompilerParams(vmem_limit_bytes=16 * MIB),
        cost_estimate=pl.CostEstimate(
            flops=2000 * units * count,
            bytes_accessed=12 * MIB,
            transcendentals=units * count,
        ),
        name="slopes",
    )(pre, unit)


def term_kernel(slope_ref, lam_ref, own_ref, other_ref, out_ref):
    count = own_ref.shape[0]
    grad_pre = (slope_ref[...] * lam_ref[...]).astype(bf16)
    out_ref[...] = (
        jnp.dot(grad_pre[:, :count], own_ref[...], preferred_element_type=f32)
        + jnp.dot(grad_pre[:, count:], other_ref[...], preferred_element_type=f32)
    ).astype(bf16)


def gradient_term(slope, lam, own, other):
    units, both = slope.shape
    count, width = own.shape
    block = units // 2
    return pl.pallas_call(
        term_kernel,
        grid=(units // block,),
        in_specs=[
            pl.BlockSpec((block, both), lambda i: (i, 0)),
            pl.BlockSpec((1, both), lambda i: (0, 0)),
            pl.BlockSpec((count, width), lambda i: (0, 0)),
            pl.BlockSpec((count, width), lambda i: (0, 0)),
        ],
        out_specs=pl.BlockSpec((block, width), lambda i: (i, 0)),
        out_shape=jax.ShapeDtypeStruct((units, width), bf16),
        compiler_params=pltpu.CompilerParams(vmem_limit_bytes=32 * MIB),
        cost_estimate=pl.CostEstimate(
            flops=2 * units * width * both, bytes_accessed=12 * MIB, transcendentals=0
        ),
        name="gradient_term",
    )(slope, lam, own, other)


def per_device(embeddings, hidden_weight, score_weight, relevance, rank_pos, ideal_dcg):
    groups, local, width = embeddings.shape
    owned_rows = hidden_weight.shape[0]
    cores = lax.axis_size("c")
    chips = lax.axis_size("y") * lax.axis_size("x")
    planes = lax.axis_size("z")
    core = lax.axis_index("c")
    chip = lax.axis_index("y") * lax.axis_size("x") + lax.axis_index("x")
    own = embeddings.reshape(groups * local, width)

    weight = spread(hidden_weight, CHIPS, chips).reshape(chips * owned_rows, width)
    other = lax.ppermute(own, "c", [(0, 1), (1, 0)])
    unit = lax.dynamic_index_in_dim(
        score_weight.reshape(chips, cores, owned_rows), core, 1, keepdims=False
    ).reshape(chips * owned_rows, 1).astype(f32)
    code = (8 * rank_pos + relevance).astype(f32)

    pre, part = score(weight, own, other, unit)
    message = jnp.concatenate([part.reshape(2, groups, local), code[None]], axis=0)
    heard = spread(message, CAND, chips * cores)
    slope = slopes(pre, unit)

    heard = heard.reshape(chips, cores, 3, groups, local)
    scores = heard[:, :, 0] + heard[:, ::-1, 1]
    rank = jnp.floor(heard[:, :, 2] * 0.125)
    gain = jnp.exp2(heard[:, :, 2] - 8.0 * rank) - 1.0
    disc = 1.0 / jnp.log2(2.0 + rank)
    facts = jnp.stack([0.5 * scores, gain, disc]).transpose(0, 3, 1, 2, 4)
    mine = lax.dynamic_index_in_dim(facts, chip, 2, keepdims=False)
    mine = mine.reshape(3, groups, cores * local)[:, :, :, None]
    facts = facts.reshape(3, groups, chips * cores * local)[:, :, None, :]
    pull = (facts[1] - mine[1]) * jnp.abs(facts[2] - mine[2])
    pair_lam = jnp.sum(pull + jnp.abs(pull) * jnp.tanh(mine[0] - facts[0]), axis=-1)
    pair_lam = (pair_lam * (0.5 / ideal_dcg)[:, None]).reshape(groups, cores, local)
    pair_lam = pair_lam.transpose(1, 0, 2)
    pair_lam = jnp.where(core == 0, pair_lam, pair_lam[::-1])
    lambdas = pair_lam[0]

    term = gradient_term(slope, pair_lam.reshape(1, -1), own, other)
    terms = lax.all_to_all(
        term.reshape(chips, owned_rows, width), CHIPS, split_axis=0, concat_axis=0, tiled=True
    )
    owned = jnp.sum(terms.astype(f32), axis=0).astype(bf16)
    pieces = lax.all_to_all(
        owned.reshape(planes, owned_rows // planes, width), "z", split_axis=0, concat_axis=0, tiled=True
    )
    piece = jnp.sum(pieces.astype(f32), axis=0).astype(bf16)
    total = spread(piece, "z", planes).reshape(owned_rows, width).astype(f32)
    squares = jnp.sum(spread(jnp.sum(total * total), CAND, chips * cores))
    entries = owned_rows * width * chips * cores
    return total * lax.rsqrt(squares / entries + EPS), lambdas


def solution(mesh):
    fine = Mesh(mesh.devices.reshape(mesh.devices.shape[0], 4, 4, 2), ("z", "y", "x", "c"))
    return jax.shard_map(
        per_device,
        mesh=fine,
        in_specs=(
            P("z", CAND, None),
            P(CAND, None),
            P(),
            P("z", CAND),
            P("z", CAND),
            P("z"),
        ),
        out_specs=(P(CAND, None), P("z", CAND)),
        check_vma=False,
    )
```

```python
import functools

import jax
import jax.numpy as jnp
from jax import lax
from jax.experimental import pallas as pl
from jax.experimental.pallas import tpu as pltpu
from jax.sharding import Mesh
from jax.sharding import PartitionSpec as P

EPS = 1e-06
GELU_A = 0.7978845608028654
GELU_B = 0.044715
CHIPS = ("y", "x")
CAND = ("y", "x", "c")
MIB = 1 << 20
LANES = 128
f32 = jnp.float32
bf16 = jnp.bfloat16


def spread(value, axis, size):
    copies = jnp.broadcast_to(value[None], (size, *value.shape))
    return lax.all_to_all(copies, axis, split_axis=0, concat_axis=0, tiled=True)


def score_kernel(weight_ref, own_ref, other_ref, unit_ref, code_ref, slope_ref, message_ref, part_ref):
    step = pl.program_id(0)

    @pl.when(step == 0)
    def _():
        part_ref[...] = jnp.zeros_like(part_ref)

    weight = weight_ref[...]
    unit = unit_ref[...]
    half_unit = 0.5 * unit
    for half, rows_ref in enumerate((own_ref, other_ref)):
        count = rows_ref.shape[0]
        for first in range(0, count, 256):
            pre = lax.dot_general(
                weight,
                rows_ref[first : first + 256, :],
                (((1,), (1,)), ((), ())),
                preferred_element_type=f32,
            )
            cols = slice(half * count + first, half * count + first + 256)
            square = pre * pre
            tanh = jnp.tanh(pre * (GELU_A + (GELU_A * GELU_B) * square))
            upper = 1.0 + tanh
            acts = ((0.5 * pre) * upper).astype(bf16).astype(f32)
            part_ref[:, cols] += jnp.sum(acts * unit, axis=0, keepdims=True)
            slope_ref[:, cols] = half_unit * (
                upper
                + pre * (1.0 - tanh * tanh) * (GELU_A + (3.0 * GELU_A * GELU_B) * square)
            )

    @pl.when(step == pl.num_programs(0) - 1)
    def _():
        row = jnp.concatenate([part_ref[...], code_ref[...]], axis=1)
        for d in range(message_ref.shape[0]):
            message_ref[d] = row


def score(weight, own, other, unit, code, devices):
    units, width = weight.shape
    count = own.shape[0]
    block = units // 2
    whole = lambda i: (0, 0)
    return pl.pallas_call(
        score_kernel,
        grid=(units // block,),
        in_specs=[
            pl.BlockSpec((block, width), lambda i: (i, 0)),
            pl.BlockSpec((count, width), whole),
            pl.BlockSpec((count, width), whole),
            pl.BlockSpec((block, 1), lambda i: (i, 0)),
            pl.BlockSpec((1, count), whole),
        ],
        out_specs=[
            pl.BlockSpec((block, 2 * count), lambda i: (i, 0)),
            pl.BlockSpec((devices, 1, 3 * count), lambda i: (0, 0, 0)),
        ],
        out_shape=[
            pltpu.HBM((units, 2 * count), f32),
            jax.ShapeDtypeStruct((devices, 1, 3 * count), f32),
        ],
        scratch_shapes=[pltpu.VMEM((1, 2 * count), f32)],
        compiler_params=pltpu.CompilerParams(vmem_limit_bytes=40 * MIB),
        cost_estimate=pl.CostEstimate(
            flops=4 * units * width * count,
            bytes_accessed=12 * MIB,
            transcendentals=2 * units * count,
        ),
        name="score",
    )(weight, own, other, unit, code)


def term_kernel(slope_ref, lam_ref, own_ref, other_ref, out_ref):
    count = own_ref.shape[0]
    out = None
    for half, rows_ref in enumerate((own_ref, other_ref)):
        grad_pre = (slope_ref[:, half * count : (half + 1) * count] * lam_ref[half : half + 1, :]).astype(bf16)
        part = jnp.dot(grad_pre, rows_ref[...], preferred_element_type=f32)
        out = part if out is None else out + part
    out_ref[...] = out.astype(bf16)


def gradient_term(slope, lam, own, other):
    units, both = slope.shape
    count, width = own.shape
    block = units // 2
    return pl.pallas_call(
        term_kernel,
        grid=(units // block,),
        in_specs=[
            pl.BlockSpec((block, both), lambda i: (i, 0)),
            pl.BlockSpec((2, count), lambda i: (0, 0)),
            pl.BlockSpec((count, width), lambda i: (0, 0)),
            pl.BlockSpec((count, width), lambda i: (0, 0)),
        ],
        out_specs=pl.BlockSpec((block, width), lambda i: (i, 0)),
        out_shape=jax.ShapeDtypeStruct((units, width), bf16),
        compiler_params=pltpu.CompilerParams(vmem_limit_bytes=32 * MIB),
        cost_estimate=pl.CostEstimate(
            flops=2 * units * width * both, bytes_accessed=12 * MIB, transcendentals=0
        ),
        name="gradient_term",
    )(slope, lam, own, other)


def pair_kernel(place_ref, heard_ref, half_ref, lam_ref, raw_ref, far_ref, own_ref, sum_ref):
    devices, _, size = heard_ref.shape
    width = size // 3
    local = 32
    for d in range(devices):
        raw_ref[d : d + 1, :] = heard_ref[d]
    row = lax.broadcasted_iota(jnp.int32, (devices, width), 0)
    near = raw_ref[:, width : 2 * width]
    near = jnp.where(row % 2 == 0, pltpu.roll(near, devices - 1, 0), pltpu.roll(near, 1, 0))
    code = raw_ref[:, 2 * width :]
    rank = jnp.floor(code * 0.125)
    level = (code - 8.0 * rank).astype(jnp.int32)
    far_ref[0] = 0.5 * (raw_ref[:, :width] + near)
    far_ref[1] = (jnp.left_shift(jnp.ones_like(level), level) - 1).astype(f32)
    far_ref[2] = 0.6931471805599453 / jnp.log(2.0 + rank)

    lane = lax.broadcasted_iota(jnp.int32, (LANES, LANES), 1)
    sub = lax.broadcasted_iota(jnp.int32, (LANES, LANES), 0)
    ones = (lane // local == sub // local).astype(f32)
    pick = lax.broadcasted_iota(jnp.int32, (local, width), 1) % local == lax.broadcasted_iota(
        jnp.int32, (local, width), 0
    )
    for c in range(2):
        mine = row == 2 * place_ref[0] + c
        for k in range(3):
            value = jnp.sum(jnp.where(mine, far_ref[k], 0.0), axis=0, keepdims=True)
            value = jnp.where(pick, value, 0.0)
            for first in range(0, width, LANES):
                at = ((first // LANES * 3 + k) * 2 + c) * local
                own_ref[at : at + local, :] = value[:, first : first + LANES]
    own_ref[...] = jnp.dot(
        own_ref[...], ones, precision=lax.Precision.HIGHEST, preferred_element_type=f32
    )
    pairs = 2 * local
    for first in range(0, width, LANES):
        cols = slice(first, first + LANES)
        at = first // LANES * 3 * pairs
        own_score, own_gain, own_disc = (
            own_ref[at + k * pairs : at + (k + 1) * pairs, :] for k in range(3)
        )

        def step(n, total):
            rows = pl.ds(pl.multiple_of(8 * n, 8), 8)
            score, gain, disc = far_ref[0, rows, cols], far_ref[1, rows, cols], far_ref[2, rows, cols]
            for j in range(8):
                gain_diff = gain[j : j + 1] - own_gain
                disc_diff = jnp.abs(disc[j : j + 1] - own_disc)
                pull = gain_diff * disc_diff
                total += pull + jnp.abs(pull) * jnp.tanh(own_score - score[j : j + 1])
            return total

        at = first // LANES * pairs
        sum_ref[at : at + pairs, :] = lax.fori_loop(0, devices // 8, step, jnp.zeros((pairs, LANES), f32))
    sum_ref[...] = jnp.dot(
        sum_ref[...], ones, precision=lax.Precision.HIGHEST, preferred_element_type=f32
    )
    for first in range(0, width, LANES):
        cols = slice(first, first + LANES)
        at = first // LANES * pairs
        lam = [
            half_ref[:, cols]
            * jnp.sum(
                jnp.where(pick[:, cols], sum_ref[at + c * local : at + (c + 1) * local, :], 0.0), axis=0, keepdims=True
            )
            for c in range(2)
        ]
        south = place_ref[1] == 0
        lam_ref[0:1, cols] = jnp.where(south, lam[0], lam[1])
        lam_ref[1:2, cols] = jnp.where(south, lam[1], lam[0])


def pair_lambdas(heard, half, place):
    devices, _, size = heard.shape
    width = size // 3
    return pl.pallas_call(
        pair_kernel,
        in_specs=[
            pl.BlockSpec(memory_space=pltpu.SMEM),
            pl.BlockSpec(memory_space=pltpu.VMEM),
            pl.BlockSpec(memory_space=pltpu.VMEM),
        ],
        out_specs=pl.BlockSpec(memory_space=pltpu.VMEM),
        out_shape=jax.ShapeDtypeStruct((2, width), f32),
        scratch_shapes=[
            pltpu.VMEM((devices, size), f32),
            pltpu.VMEM((3, devices, width), f32),
            pltpu.VMEM((width // LANES * 6 * 32, LANES), f32),
            pltpu.VMEM((width // LANES * 2 * 32, LANES), f32),
        ],
        compiler_params=pltpu.CompilerParams(vmem_limit_bytes=16 * MIB),
        cost_estimate=pl.CostEstimate(flops=2 * MIB * 10, bytes_accessed=MIB, transcendentals=2 * MIB),
        name="pair_lambdas",
    )(place, heard, half)


def copies_kernel(block_ref, out_ref):
    for k in range(out_ref.shape[0]):
        out_ref[k] = block_ref[...]


def copies(block, count):
    rows, width = block.shape
    step = count // 4
    return pl.pallas_call(
        copies_kernel,
        grid=(count // step,),
        in_specs=[pl.BlockSpec((rows, width), lambda i: (0, 0))],
        out_specs=pl.BlockSpec((step, rows, width), lambda i: (i, 0, 0)),
        out_shape=jax.ShapeDtypeStruct((count, rows, width), block.dtype),
        compiler_params=pltpu.CompilerParams(vmem_limit_bytes=16 * MIB),
        name="copies",
    )(block)


def squares_kernel(total_ref, out_ref):
    total = total_ref[...].astype(f32)
    square = jnp.sum(total * total, axis=0)
    square = jnp.sum(jnp.sum(square, axis=0, keepdims=True), axis=1, keepdims=True)
    row = jnp.broadcast_to(square, (1, LANES))
    for d in range(out_ref.shape[0]):
        out_ref[d] = row


def squares(total, devices):
    return pl.pallas_call(
        squares_kernel,
        in_specs=[pl.BlockSpec(memory_space=pltpu.VMEM)],
        out_specs=pl.BlockSpec(memory_space=pltpu.VMEM),
        out_shape=jax.ShapeDtypeStruct((devices, 1, LANES), f32),
        compiler_params=pltpu.CompilerParams(vmem_limit_bytes=16 * MIB),
        name="squares",
    )(total)


def scaled_kernel(entries, total_ref, heard_ref, out_ref):
    square = jnp.sum(heard_ref[...], axis=0)
    scale = lax.rsqrt(square * (1.0 / entries) + EPS)
    planes, rows, cut = total_ref.shape
    across = out_ref.shape[1] // cut
    scale = jnp.concatenate([scale] * (cut // LANES), axis=1)
    for k in range(planes):
        at, col = k // across * rows, k % across * cut
        out_ref[at : at + rows, col : col + cut] = total_ref[k].astype(f32) * scale


def scaled(total, heard, rows, width, entries):
    return pl.pallas_call(
        functools.partial(scaled_kernel, entries),
        in_specs=[pl.BlockSpec(memory_space=pltpu.VMEM)] * 2,
        out_specs=pl.BlockSpec(memory_space=pltpu.VMEM),
        out_shape=jax.ShapeDtypeStruct((rows, width), f32),
        compiler_params=pltpu.CompilerParams(vmem_limit_bytes=16 * MIB),
        name="scaled",
    )(total, heard)


def per_device(embeddings, hidden_weight, score_weight, relevance, rank_pos, ideal_dcg):
    groups, local, width = embeddings.shape
    owned_rows = hidden_weight.shape[0]
    cores = lax.axis_size("c")
    chips = lax.axis_size("y") * lax.axis_size("x")
    planes = lax.axis_size("z")
    core = lax.axis_index("c")
    chip = lax.axis_index("y") * lax.axis_size("x") + lax.axis_index("x")
    own = embeddings.reshape(groups * local, width)

    weight = lax.all_to_all(
        copies(hidden_weight, chips), CHIPS, split_axis=0, concat_axis=0, tiled=True
    ).reshape(chips * owned_rows, width)
    other = lax.ppermute(own, "c", [(0, 1), (1, 0)])
    unit = lax.dynamic_index_in_dim(
        score_weight.reshape(chips, cores, owned_rows), core, 1, keepdims=False
    ).reshape(chips * owned_rows, 1).astype(f32)
    code = (8 * rank_pos + relevance).astype(f32).reshape(1, groups * local)
    half = jnp.repeat(0.5 / ideal_dcg, local).reshape(1, groups * local)
    place = jnp.stack([chip, core]).astype(jnp.int32)

    slope, message = score(weight, own, other, unit, code, chips * cores)
    heard = lax.all_to_all(message, CAND, split_axis=0, concat_axis=0, tiled=True)
    lam = pair_lambdas(heard, half, place)
    lambdas = lam[0].reshape(groups, local)

    term = gradient_term(slope, lam, own, other)
    terms = lax.all_to_all(
        term.reshape(chips, owned_rows, width), CHIPS, split_axis=0, concat_axis=0, tiled=True
    )
    owned = jnp.sum(terms.astype(f32), axis=0).astype(bf16)
    across = planes * 8 // owned_rows
    owned = owned.reshape(owned_rows // 8, 8, across, width // across).transpose(0, 2, 1, 3)
    pieces = lax.all_to_all(
        owned.reshape(planes, 8, width // across), "z", split_axis=0, concat_axis=0, tiled=True
    )
    piece = jnp.sum(pieces.astype(f32), axis=0).astype(bf16)
    total = spread(piece, "z", planes)
    entries = owned_rows * width * chips * cores
    square = lax.all_to_all(
        squares(total, chips * cores), CAND, split_axis=0, concat_axis=0, tiled=True
    )
    return scaled(total, square, owned_rows, width, entries), lambdas


def solution(mesh):
    fine = Mesh(mesh.devices.reshape(mesh.devices.shape[0], 4, 4, 2), ("z", "y", "x", "c"))
    return jax.shard_map(
        per_device,
        mesh=fine,
        in_specs=(
            P("z", CAND, None),
            P(CAND, None),
            P(),
            P("z", CAND),
            P("z", CAND),
            P("z"),
        ),
        out_specs=(P(CAND, None), P("z", CAND)),
        check_vma=False,
    )
```

```python
import functools

import jax
import jax.numpy as jnp
from jax import lax
from jax.experimental import pallas as pl
from jax.experimental.pallas import tpu as pltpu
from jax.sharding import Mesh
from jax.sharding import PartitionSpec as P

EPS = 1e-06
GELU_A = 0.7978845608028654
GELU_B = 0.044715
CHIPS = ("y", "x")
CAND = ("y", "x", "c")
MIB = 1 << 20
LANES = 128
f32 = jnp.float32
bf16 = jnp.bfloat16


def in_hbm(*values):
    return tuple(pltpu.with_memory_space_constraint(v, pltpu.HBM) for v in values)


def spread(value, axis, size):
    copies = jnp.broadcast_to(value[None], (size, *value.shape))
    return lax.all_to_all(copies, axis, split_axis=0, concat_axis=0, tiled=True)


def score_kernel(
    weight_ref, own_hbm, other_hbm, unit_ref, code_ref, slope_hbm, message_ref,
    rows_ref, slope_ref, part_ref, in_sems, out_sems,
):
    count = own_hbm.shape[0]
    units = weight_ref.shape[0]
    cut = rows_ref.shape[1]
    chunks = 2 * count // cut

    def fetch(n):
        source = own_hbm if n * cut < count else other_hbm
        first = n * cut % count
        return pltpu.make_async_copy(source.at[pl.ds(first, cut), :], rows_ref.at[n], in_sems.at[n])

    def put(n):
        cols = pl.ds(n * cut, cut)
        return pltpu.make_async_copy(slope_ref.at[:, cols], slope_hbm.at[:, cols], out_sems.at[n])

    for n in range(chunks):
        fetch(n).start()
    block = units // 2
    for n in range(chunks):
        fetch(n).wait()
        cols = slice(n * cut, (n + 1) * cut)
        part = jnp.zeros((1, cut), f32)
        for first in range(0, units, block):
            here = slice(first, first + block)
            unit = unit_ref[here, :]
            pre = lax.dot_general(
                weight_ref[here, :],
                rows_ref[n],
                (((1,), (1,)), ((), ())),
                preferred_element_type=f32,
            )
            square = pre * pre
            tanh = jnp.tanh(pre * (GELU_A + (GELU_A * GELU_B) * square))
            upper = 1.0 + tanh
            acts = ((0.5 * pre) * upper).astype(bf16).astype(f32)
            part += jnp.sum(acts * unit, axis=0, keepdims=True)
            slope_ref[here, cols] = (0.5 * unit) * (
                upper
                + pre * (1.0 - tanh * tanh) * (GELU_A + (3.0 * GELU_A * GELU_B) * square)
            )
        part_ref[:, cols] = part
        put(n).start()
    row = jnp.concatenate([part_ref[...], code_ref[...]], axis=1)
    for d in range(message_ref.shape[0]):
        message_ref[d] = row
    for n in range(chunks):
        put(n).wait()


def score(weight, own, other, unit, code, devices):
    units, width = weight.shape
    count = own.shape[0]
    cut = 256
    chunks = 2 * count // cut
    vmem = pl.BlockSpec(memory_space=pltpu.VMEM)
    hbm = pl.BlockSpec(memory_space=pltpu.HBM)
    return pl.pallas_call(
        score_kernel,
        in_specs=[vmem, hbm, hbm, vmem, vmem],
        out_specs=[hbm, vmem],
        out_shape=[
            pltpu.HBM((units, 2 * count), f32),
            jax.ShapeDtypeStruct((devices, 1, 3 * count), f32),
        ],
        scratch_shapes=[
            pltpu.VMEM((chunks, cut, width), bf16),
            pltpu.VMEM((units, 2 * count), f32),
            pltpu.VMEM((1, 2 * count), f32),
            pltpu.SemaphoreType.DMA((chunks,)),
            pltpu.SemaphoreType.DMA((chunks,)),
        ],
        compiler_params=pltpu.CompilerParams(vmem_limit_bytes=40 * MIB),
        cost_estimate=pl.CostEstimate(
            flops=4 * units * width * count,
            bytes_accessed=12 * MIB,
            transcendentals=2 * units * count,
        ),
        name="score",
    )(weight, *in_hbm(own, other), unit, code)


def term_kernel(
    place_ref, heard_ref, half_ref, slope_hbm, own_hbm, other_hbm, lam_ref, term_ref,
    raw_ref, far_ref, own_ref, sum_ref, slope_ref, rows_ref, sems,
):
    count = own_hbm.shape[0]
    units = slope_hbm.shape[0]
    block = units // 2
    fetches = [
        pltpu.make_async_copy(own_hbm, rows_ref.at[0], sems.at[0]),
        pltpu.make_async_copy(other_hbm, rows_ref.at[1], sems.at[1]),
        pltpu.make_async_copy(slope_hbm, slope_ref, sems.at[2]),
    ]
    for fetch in fetches:
        fetch.start()
    devices, _, size = heard_ref.shape
    width = size // 3
    local = 32
    for d in range(devices):
        raw_ref[d : d + 1, :] = heard_ref[d]
    row = lax.broadcasted_iota(jnp.int32, (devices, width), 0)
    near = raw_ref[:, width : 2 * width]
    near = jnp.where(row % 2 == 0, pltpu.roll(near, devices - 1, 0), pltpu.roll(near, 1, 0))
    code = raw_ref[:, 2 * width :]
    rank = jnp.floor(code * 0.125)
    level = (code - 8.0 * rank).astype(jnp.int32)
    far_ref[0] = 0.5 * (raw_ref[:, :width] + near)
    far_ref[1] = (jnp.left_shift(jnp.ones_like(level), level) - 1).astype(f32)
    far_ref[2] = 0.6931471805599453 / jnp.log(2.0 + rank)

    lane = lax.broadcasted_iota(jnp.int32, (LANES, LANES), 1)
    sub = lax.broadcasted_iota(jnp.int32, (LANES, LANES), 0)
    ones = (lane // local == sub // local).astype(f32)
    pick = lax.broadcasted_iota(jnp.int32, (local, width), 1) % local == lax.broadcasted_iota(
        jnp.int32, (local, width), 0
    )
    for c in range(2):
        mine = row == 2 * place_ref[0] + c
        for k in range(3):
            value = jnp.sum(jnp.where(mine, far_ref[k], 0.0), axis=0, keepdims=True)
            value = jnp.where(pick, value, 0.0)
            for first in range(0, width, LANES):
                at = ((first // LANES * 3 + k) * 2 + c) * local
                own_ref[at : at + local, :] = value[:, first : first + LANES]
    own_ref[...] = jnp.dot(
        own_ref[...], ones, precision=lax.Precision.HIGHEST, preferred_element_type=f32
    )
    pairs = 2 * local
    for first in range(0, width, LANES):
        cols = slice(first, first + LANES)
        at = first // LANES * 3 * pairs
        own_score, own_gain, own_disc = (
            own_ref[at + k * pairs : at + (k + 1) * pairs, :] for k in range(3)
        )

        def step(n, total):
            rows = pl.ds(pl.multiple_of(8 * n, 8), 8)
            score, gain, disc = far_ref[0, rows, cols], far_ref[1, rows, cols], far_ref[2, rows, cols]
            for j in range(8):
                gain_diff = gain[j : j + 1] - own_gain
                disc_diff = jnp.abs(disc[j : j + 1] - own_disc)
                pull = gain_diff * disc_diff
                total += pull + jnp.abs(pull) * jnp.tanh(own_score - score[j : j + 1])
            return total

        at = first // LANES * pairs
        sum_ref[at : at + pairs, :] = lax.fori_loop(0, devices // 8, step, jnp.zeros((pairs, LANES), f32))
    sum_ref[...] = jnp.dot(
        sum_ref[...], ones, precision=lax.Precision.HIGHEST, preferred_element_type=f32
    )
    for first in range(0, width, LANES):
        cols = slice(first, first + LANES)
        at = first // LANES * pairs
        lam = [
            half_ref[:, cols]
            * jnp.sum(
                jnp.where(pick[:, cols], sum_ref[at + c * local : at + (c + 1) * local, :], 0.0), axis=0, keepdims=True
            )
            for c in range(2)
        ]
        south = place_ref[1] == 0
        lam_ref[0:1, cols] = jnp.where(south, lam[0], lam[1])
        lam_ref[1:2, cols] = jnp.where(south, lam[1], lam[0])
    for fetch in fetches:
        fetch.wait()
    for first in range(0, units, block):
        here = slice(first, first + block)
        term = None
        for k in range(2):
            slope = slope_ref[here, k * count : (k + 1) * count]
            grad_pre = (slope * lam_ref[k : k + 1, :]).astype(bf16)
            part = jnp.dot(grad_pre, rows_ref[k], preferred_element_type=f32)
            term = part if term is None else term + part
        term_ref[here, :] = term.astype(bf16)


def gradient_term(heard, half, place, slope, own, other):
    devices, _, size = heard.shape
    units = slope.shape[0]
    count, width = own.shape
    pairs = 64 * (count // LANES)
    vmem = pl.BlockSpec(memory_space=pltpu.VMEM)
    hbm = pl.BlockSpec(memory_space=pltpu.HBM)
    return pl.pallas_call(
        term_kernel,
        in_specs=[pl.BlockSpec(memory_space=pltpu.SMEM), vmem, vmem, hbm, hbm, hbm],
        out_specs=[vmem, vmem],
        out_shape=[
            jax.ShapeDtypeStruct((2, count), f32),
            jax.ShapeDtypeStruct((units, width), bf16),
        ],
        scratch_shapes=[
            pltpu.VMEM((devices, size), f32),
            pltpu.VMEM((3, devices, count), f32),
            pltpu.VMEM((3 * pairs, LANES), f32),
            pltpu.VMEM((pairs, LANES), f32),
            pltpu.VMEM(slope.shape, f32),
            pltpu.VMEM((2, count, width), bf16),
            pltpu.SemaphoreType.DMA((3,)),
        ],
        compiler_params=pltpu.CompilerParams(vmem_limit_bytes=40 * MIB),
        cost_estimate=pl.CostEstimate(
            flops=4 * units * width * count, bytes_accessed=12 * MIB, transcendentals=2 * MIB
        ),
        name="gradient_term",
    )(place, heard, half, *in_hbm(slope, own, other))


def copies_kernel(block_hbm, out_hbm, block_ref, in_sem, out_sems):
    fetch = pltpu.make_async_copy(block_hbm, block_ref, in_sem)
    fetch.start()
    fetch.wait()
    puts = [
        pltpu.make_async_copy(block_ref, out_hbm.at[k], out_sems.at[k])
        for k in range(out_hbm.shape[0])
    ]
    for put in puts:
        put.start()
    for put in puts:
        put.wait()


def copies(block, count):
    hbm = pl.BlockSpec(memory_space=pltpu.HBM)
    return pl.pallas_call(
        copies_kernel,
        in_specs=[hbm],
        out_specs=hbm,
        out_shape=pltpu.HBM((count, *block.shape), block.dtype),
        scratch_shapes=[
            pltpu.VMEM(block.shape, block.dtype),
            pltpu.SemaphoreType.DMA,
            pltpu.SemaphoreType.DMA((count,)),
        ],
        compiler_params=pltpu.CompilerParams(vmem_limit_bytes=16 * MIB),
        name="copies",
    )(*in_hbm(block))


def squares_kernel(total_ref, out_ref):
    total = total_ref[...].astype(f32)
    square = jnp.sum(total * total, axis=0)
    square = jnp.sum(jnp.sum(square, axis=0, keepdims=True), axis=1, keepdims=True)
    row = jnp.broadcast_to(square, (1, LANES))
    for d in range(out_ref.shape[0]):
        out_ref[d] = row


def squares(total, devices):
    return pl.pallas_call(
        squares_kernel,
        in_specs=[pl.BlockSpec(memory_space=pltpu.VMEM)],
        out_specs=pl.BlockSpec(memory_space=pltpu.VMEM),
        out_shape=jax.ShapeDtypeStruct((devices, 1, LANES), f32),
        compiler_params=pltpu.CompilerParams(vmem_limit_bytes=16 * MIB),
        name="squares",
    )(total)


def scaled_kernel(entries, total_ref, heard_ref, out_ref):
    square = jnp.sum(heard_ref[...], axis=0)
    scale = lax.rsqrt(square * (1.0 / entries) + EPS)
    planes, rows, cut = total_ref.shape
    across = out_ref.shape[1] // cut
    scale = jnp.concatenate([scale] * (cut // LANES), axis=1)
    for k in range(planes):
        at, col = k // across * rows, k % across * cut
        out_ref[at : at + rows, col : col + cut] = total_ref[k].astype(f32) * scale


def scaled(total, heard, rows, width, entries):
    return pl.pallas_call(
        functools.partial(scaled_kernel, entries),
        in_specs=[pl.BlockSpec(memory_space=pltpu.VMEM)] * 2,
        out_specs=pl.BlockSpec(memory_space=pltpu.VMEM),
        out_shape=jax.ShapeDtypeStruct((rows, width), f32),
        compiler_params=pltpu.CompilerParams(vmem_limit_bytes=16 * MIB),
        name="scaled",
    )(total, heard)


def per_device(embeddings, hidden_weight, score_weight, relevance, rank_pos, ideal_dcg):
    groups, local, width = embeddings.shape
    owned_rows = hidden_weight.shape[0]
    cores = lax.axis_size("c")
    chips = lax.axis_size("y") * lax.axis_size("x")
    planes = lax.axis_size("z")
    core = lax.axis_index("c")
    chip = lax.axis_index("y") * lax.axis_size("x") + lax.axis_index("x")
    own = embeddings.reshape(groups * local, width)

    weight = lax.all_to_all(
        copies(hidden_weight, chips), CHIPS, split_axis=0, concat_axis=0, tiled=True
    ).reshape(chips * owned_rows, width)
    other = lax.ppermute(own, "c", [(0, 1), (1, 0)])
    unit = lax.dynamic_index_in_dim(
        score_weight.reshape(chips, cores, owned_rows), core, 1, keepdims=False
    ).reshape(chips * owned_rows, 1).astype(f32)
    code = (8 * rank_pos + relevance).astype(f32).reshape(1, groups * local)
    half = jnp.repeat(0.5 / ideal_dcg, local).reshape(1, groups * local)
    place = jnp.stack([chip, core]).astype(jnp.int32)

    slope, message = score(weight, own, other, unit, code, chips * cores)
    heard = lax.all_to_all(message, CAND, split_axis=0, concat_axis=0, tiled=True)
    lam, term = gradient_term(heard, half, place, slope, own, other)
    lambdas = lam[0].reshape(groups, local)
    terms = lax.all_to_all(
        term.reshape(chips, owned_rows, width), CHIPS, split_axis=0, concat_axis=0, tiled=True
    )
    owned = jnp.sum(terms.astype(f32), axis=0).astype(bf16)
    across = planes * 8 // owned_rows
    owned = owned.reshape(owned_rows // 8, 8, across, width // across).transpose(0, 2, 1, 3)
    pieces = lax.all_to_all(
        owned.reshape(planes, 8, width // across), "z", split_axis=0, concat_axis=0, tiled=True
    )
    piece = jnp.sum(pieces.astype(f32), axis=0).astype(bf16)
    total = spread(piece, "z", planes)
    entries = owned_rows * width * chips * cores
    square = lax.all_to_all(
        squares(total, chips * cores), CAND, split_axis=0, concat_axis=0, tiled=True
    )
    return scaled(total, square, owned_rows, width, entries), lambdas


def solution(mesh):
    fine = Mesh(mesh.devices.reshape(mesh.devices.shape[0], 4, 4, 2), ("z", "y", "x", "c"))
    return jax.shard_map(
        per_device,
        mesh=fine,
        in_specs=(
            P("z", CAND, None),
            P(CAND, None),
            P(),
            P("z", CAND),
            P("z", CAND),
            P("z"),
        ),
        out_specs=(P(CAND, None), P("z", CAND)),
        check_vma=False,
    )
```

```python
import functools

import jax
import jax.numpy as jnp
from jax import lax
from jax.experimental import pallas as pl
from jax.experimental.pallas import tpu as pltpu
from jax.sharding import Mesh
from jax.sharding import PartitionSpec as P

EPS = 1e-06
GELU_A = 0.7978845608028654
GELU_B = 0.044715
CHIPS = ("y", "x")
CAND = ("y", "x", "c")
MIB = 1 << 20
LANES = 128
f32 = jnp.float32
bf16 = jnp.bfloat16


def in_hbm(*values):
    return tuple(pltpu.with_memory_space_constraint(v, pltpu.HBM) for v in values)


def spread(value, axis, size):
    copies = jnp.broadcast_to(value[None], (size, *value.shape))
    return lax.all_to_all(copies, axis, split_axis=0, concat_axis=0, tiled=True)


def score_kernel(
    weight_ref, own_hbm, other_hbm, unit_ref, code_ref, slope_hbm, message_ref,
    rows_ref, slope_ref, part_ref, in_sems, out_sems,
):
    count = own_hbm.shape[0]
    units = weight_ref.shape[0]
    cut = rows_ref.shape[1]
    chunks = 2 * count // cut

    def fetch(n):
        source = own_hbm if n * cut < count else other_hbm
        first = n * cut % count
        return pltpu.make_async_copy(source.at[pl.ds(first, cut), :], rows_ref.at[n], in_sems.at[n])

    def put(n):
        cols = pl.ds(n * cut, cut)
        return pltpu.make_async_copy(slope_ref.at[:, cols], slope_hbm.at[:, cols], out_sems.at[n])

    for n in range(chunks):
        fetch(n).start()
    block = 512
    tiles = [(n, first) for n in range(chunks) for first in range(0, units, block)]

    def product(n, first):
        if first == 0:
            fetch(n).wait()
        return lax.dot_general(
            weight_ref[first : first + block, :],
            rows_ref[n],
            (((1,), (1,)), ((), ())),
            preferred_element_type=f32,
        )

    ahead = product(*tiles[0])
    for at, (n, first) in enumerate(tiles):
        pre = ahead
        if at + 1 < len(tiles):
            ahead = product(*tiles[at + 1])
        here = slice(first, first + block)
        cols = slice(n * cut, (n + 1) * cut)
        half_unit = 0.5 * unit_ref[here, :]
        line = GELU_A * pre
        cube = (GELU_B * (pre * pre)) * line
        inner = line + cube
        tanh = jnp.tanh(inner)
        upper = 1.0 + tanh
        acts = (pre * upper).astype(bf16).astype(f32)
        part = jnp.sum(acts * half_unit, axis=0, keepdims=True)
        part_ref[:, cols] = part if first == 0 else part_ref[:, cols] + part
        slope_ref[here, cols] = half_unit * (
            upper + (1.0 - tanh * tanh) * (inner + (cube + cube))
        )
        if first + block == units:
            put(n).start()
    row = jnp.concatenate([part_ref[...], code_ref[...]], axis=1)
    for d in range(message_ref.shape[0]):
        message_ref[d] = row
    for n in range(chunks):
        put(n).wait()


def score(weight, own, other, unit, code, devices):
    units, width = weight.shape
    count = own.shape[0]
    cut = 256
    chunks = 2 * count // cut
    vmem = pl.BlockSpec(memory_space=pltpu.VMEM)
    hbm = pl.BlockSpec(memory_space=pltpu.HBM)
    return pl.pallas_call(
        score_kernel,
        in_specs=[vmem, hbm, hbm, vmem, vmem],
        out_specs=[hbm, vmem],
        out_shape=[
            pltpu.HBM((units, 2 * count), f32),
            jax.ShapeDtypeStruct((devices, 1, 3 * count), f32),
        ],
        scratch_shapes=[
            pltpu.VMEM((chunks, cut, width), bf16),
            pltpu.VMEM((units, 2 * count), f32),
            pltpu.VMEM((1, 2 * count), f32),
            pltpu.SemaphoreType.DMA((chunks,)),
            pltpu.SemaphoreType.DMA((chunks,)),
        ],
        compiler_params=pltpu.CompilerParams(vmem_limit_bytes=40 * MIB),
        cost_estimate=pl.CostEstimate(
            flops=4 * units * width * count,
            bytes_accessed=12 * MIB,
            transcendentals=2 * units * count,
        ),
        name="score",
    )(weight, *in_hbm(own, other), unit, code)


def term_kernel(
    place_ref, heard_ref, half_ref, slope_hbm, own_hbm, other_hbm, lam_ref, term_ref,
    raw_ref, far_ref, own_ref, sum_ref, slope_ref, rows_ref, sems,
):
    count = own_hbm.shape[0]
    units = slope_hbm.shape[0]
    block = units // 2
    fetches = [
        pltpu.make_async_copy(own_hbm, rows_ref.at[0], sems.at[0]),
        pltpu.make_async_copy(other_hbm, rows_ref.at[1], sems.at[1]),
        pltpu.make_async_copy(slope_hbm, slope_ref, sems.at[2]),
    ]
    for fetch in fetches:
        fetch.start()
    devices, _, size = heard_ref.shape
    width = size // 3
    local = 32
    for d in range(devices):
        raw_ref[d : d + 1, :] = heard_ref[d]
    row = lax.broadcasted_iota(jnp.int32, (devices, width), 0)
    near = raw_ref[:, width : 2 * width]
    near = jnp.where(row % 2 == 0, pltpu.roll(near, devices - 1, 0), pltpu.roll(near, 1, 0))
    code = raw_ref[:, 2 * width :]
    rank = jnp.floor(code * 0.125)
    level = (code - 8.0 * rank).astype(jnp.int32)
    far_ref[0] = 0.5 * (raw_ref[:, :width] + near)
    far_ref[1] = (jnp.left_shift(jnp.ones_like(level), level) - 1).astype(f32)
    far_ref[2] = 0.6931471805599453 / jnp.log(2.0 + rank)

    lane = lax.broadcasted_iota(jnp.int32, (LANES, LANES), 1)
    sub = lax.broadcasted_iota(jnp.int32, (LANES, LANES), 0)
    ones = (lane // local == sub // local).astype(f32)
    pick = lax.broadcasted_iota(jnp.int32, (local, width), 1) % local == lax.broadcasted_iota(
        jnp.int32, (local, width), 0
    )
    for c in range(2):
        mine = row == 2 * place_ref[0] + c
        for k in range(3):
            value = jnp.sum(jnp.where(mine, far_ref[k], 0.0), axis=0, keepdims=True)
            value = jnp.where(pick, value, 0.0)
            for first in range(0, width, LANES):
                at = ((first // LANES * 3 + k) * 2 + c) * local
                own_ref[at : at + local, :] = value[:, first : first + LANES]
    own_ref[...] = jnp.dot(
        own_ref[...], ones, precision=lax.Precision.HIGHEST, preferred_element_type=f32
    )
    pairs = 2 * local
    for first in range(0, width, LANES):
        cols = slice(first, first + LANES)
        at = first // LANES * 3 * pairs
        own_score, own_gain, own_disc = (
            own_ref[at + k * pairs : at + (k + 1) * pairs, :] for k in range(3)
        )

        def step(n, total):
            rows = pl.ds(pl.multiple_of(8 * n, 8), 8)
            score, gain, disc = far_ref[0, rows, cols], far_ref[1, rows, cols], far_ref[2, rows, cols]
            for j in range(8):
                gain_diff = gain[j : j + 1] - own_gain
                disc_diff = jnp.abs(disc[j : j + 1] - own_disc)
                pull = gain_diff * disc_diff
                total += pull + jnp.abs(pull) * jnp.tanh(own_score - score[j : j + 1])
            return total

        at = first // LANES * pairs
        sum_ref[at : at + pairs, :] = lax.fori_loop(0, devices // 8, step, jnp.zeros((pairs, LANES), f32))
    sum_ref[...] = jnp.dot(
        sum_ref[...], ones, precision=lax.Precision.HIGHEST, preferred_element_type=f32
    )
    for first in range(0, width, LANES):
        cols = slice(first, first + LANES)
        at = first // LANES * pairs
        lam = [
            half_ref[:, cols]
            * jnp.sum(
                jnp.where(pick[:, cols], sum_ref[at + c * local : at + (c + 1) * local, :], 0.0), axis=0, keepdims=True
            )
            for c in range(2)
        ]
        south = place_ref[1] == 0
        lam_ref[0:1, cols] = jnp.where(south, lam[0], lam[1])
        lam_ref[1:2, cols] = jnp.where(south, lam[1], lam[0])
    for fetch in fetches:
        fetch.wait()
    for first in range(0, units, block):
        here = slice(first, first + block)
        term = None
        for k in range(2):
            slope = slope_ref[here, k * count : (k + 1) * count]
            grad_pre = (slope * lam_ref[k : k + 1, :]).astype(bf16)
            part = jnp.dot(grad_pre, rows_ref[k], preferred_element_type=f32)
            term = part if term is None else term + part
        term_ref[here, :] = term.astype(bf16)


def gradient_term(heard, half, place, slope, own, other):
    devices, _, size = heard.shape
    units = slope.shape[0]
    count, width = own.shape
    pairs = 64 * (count // LANES)
    vmem = pl.BlockSpec(memory_space=pltpu.VMEM)
    hbm = pl.BlockSpec(memory_space=pltpu.HBM)
    return pl.pallas_call(
        term_kernel,
        in_specs=[pl.BlockSpec(memory_space=pltpu.SMEM), vmem, vmem, hbm, hbm, hbm],
        out_specs=[vmem, vmem],
        out_shape=[
            jax.ShapeDtypeStruct((2, count), f32),
            jax.ShapeDtypeStruct((units, width), bf16),
        ],
        scratch_shapes=[
            pltpu.VMEM((devices, size), f32),
            pltpu.VMEM((3, devices, count), f32),
            pltpu.VMEM((3 * pairs, LANES), f32),
            pltpu.VMEM((pairs, LANES), f32),
            pltpu.VMEM(slope.shape, f32),
            pltpu.VMEM((2, count, width), bf16),
            pltpu.SemaphoreType.DMA((3,)),
        ],
        compiler_params=pltpu.CompilerParams(vmem_limit_bytes=40 * MIB),
        cost_estimate=pl.CostEstimate(
            flops=4 * units * width * count, bytes_accessed=12 * MIB, transcendentals=2 * MIB
        ),
        name="gradient_term",
    )(place, heard, half, *in_hbm(slope, own, other))


def copies_kernel(block_hbm, out_hbm, block_ref, in_sem, out_sems):
    fetch = pltpu.make_async_copy(block_hbm, block_ref, in_sem)
    fetch.start()
    fetch.wait()
    puts = [
        pltpu.make_async_copy(block_ref, out_hbm.at[k], out_sems.at[k])
        for k in range(out_hbm.shape[0])
    ]
    for put in puts:
        put.start()
    for put in puts:
        put.wait()


def copies(block, count):
    hbm = pl.BlockSpec(memory_space=pltpu.HBM)
    return pl.pallas_call(
        copies_kernel,
        in_specs=[hbm],
        out_specs=hbm,
        out_shape=pltpu.HBM((count, *block.shape), block.dtype),
        scratch_shapes=[
            pltpu.VMEM(block.shape, block.dtype),
            pltpu.SemaphoreType.DMA,
            pltpu.SemaphoreType.DMA((count,)),
        ],
        compiler_params=pltpu.CompilerParams(vmem_limit_bytes=16 * MIB),
        name="copies",
    )(*in_hbm(block))


def squares_kernel(total_ref, out_ref):
    total = total_ref[...].astype(f32)
    square = jnp.sum(total * total, axis=0)
    square = jnp.sum(jnp.sum(square, axis=0, keepdims=True), axis=1, keepdims=True)
    row = jnp.broadcast_to(square, (1, LANES))
    for d in range(out_ref.shape[0]):
        out_ref[d] = row


def squares(total, devices):
    return pl.pallas_call(
        squares_kernel,
        in_specs=[pl.BlockSpec(memory_space=pltpu.VMEM)],
        out_specs=pl.BlockSpec(memory_space=pltpu.VMEM),
        out_shape=jax.ShapeDtypeStruct((devices, 1, LANES), f32),
        compiler_params=pltpu.CompilerParams(vmem_limit_bytes=16 * MIB),
        name="squares",
    )(total)


def scaled_kernel(entries, total_ref, heard_ref, out_ref):
    square = jnp.sum(heard_ref[...], axis=0)
    scale = lax.rsqrt(square * (1.0 / entries) + EPS)
    planes, rows, cut = total_ref.shape
    across = out_ref.shape[1] // cut
    scale = jnp.concatenate([scale] * (cut // LANES), axis=1)
    for k in range(planes):
        at, col = k // across * rows, k % across * cut
        out_ref[at : at + rows, col : col + cut] = total_ref[k].astype(f32) * scale


def scaled(total, heard, rows, width, entries):
    return pl.pallas_call(
        functools.partial(scaled_kernel, entries),
        in_specs=[pl.BlockSpec(memory_space=pltpu.VMEM)] * 2,
        out_specs=pl.BlockSpec(memory_space=pltpu.VMEM),
        out_shape=jax.ShapeDtypeStruct((rows, width), f32),
        compiler_params=pltpu.CompilerParams(vmem_limit_bytes=16 * MIB),
        name="scaled",
    )(total, heard)


def per_device(embeddings, hidden_weight, score_weight, relevance, rank_pos, ideal_dcg):
    groups, local, width = embeddings.shape
    owned_rows = hidden_weight.shape[0]
    cores = lax.axis_size("c")
    chips = lax.axis_size("y") * lax.axis_size("x")
    planes = lax.axis_size("z")
    core = lax.axis_index("c")
    chip = lax.axis_index("y") * lax.axis_size("x") + lax.axis_index("x")
    own = embeddings.reshape(groups * local, width)

    weight = lax.all_to_all(
        copies(hidden_weight, chips), CHIPS, split_axis=0, concat_axis=0, tiled=True
    ).reshape(chips * owned_rows, width)
    other = lax.ppermute(own, "c", [(0, 1), (1, 0)])
    unit = lax.dynamic_index_in_dim(
        score_weight.reshape(chips, cores, owned_rows), core, 1, keepdims=False
    ).reshape(chips * owned_rows, 1).astype(f32)
    code = (8 * rank_pos + relevance).astype(f32).reshape(1, groups * local)
    half = jnp.repeat(0.5 / ideal_dcg, local).reshape(1, groups * local)
    place = jnp.stack([chip, core]).astype(jnp.int32)

    slope, message = score(weight, own, other, unit, code, chips * cores)
    heard = lax.all_to_all(message, CAND, split_axis=0, concat_axis=0, tiled=True)
    lam, term = gradient_term(heard, half, place, slope, own, other)
    lambdas = lam[0].reshape(groups, local)
    terms = lax.all_to_all(
        term.reshape(chips, owned_rows, width), CHIPS, split_axis=0, concat_axis=0, tiled=True
    )
    owned = jnp.sum(terms.astype(f32), axis=0).astype(bf16)
    across = planes * 8 // owned_rows
    owned = owned.reshape(owned_rows // 8, 8, across, width // across).transpose(0, 2, 1, 3)
    pieces = lax.all_to_all(
        owned.reshape(planes, 8, width // across), "z", split_axis=0, concat_axis=0, tiled=True
    )
    piece = jnp.sum(pieces.astype(f32), axis=0).astype(bf16)
    total = spread(piece, "z", planes)
    entries = owned_rows * width * chips * cores
    square = lax.all_to_all(
        squares(total, chips * cores), CAND, split_axis=0, concat_axis=0, tiled=True
    )
    return scaled(total, square, owned_rows, width, entries), lambdas


def solution(mesh):
    fine = Mesh(mesh.devices.reshape(mesh.devices.shape[0], 4, 4, 2), ("z", "y", "x", "c"))
    return jax.shard_map(
        per_device,
        mesh=fine,
        in_specs=(
            P("z", CAND, None),
            P(CAND, None),
            P(),
            P("z", CAND),
            P("z", CAND),
            P("z"),
        ),
        out_specs=(P(CAND, None), P("z", CAND)),
        check_vma=False,
    )
```

```python
import functools

import jax
import jax.numpy as jnp
from jax import lax
from jax.experimental import pallas as pl
from jax.experimental.pallas import tpu as pltpu
from jax.sharding import Mesh
from jax.sharding import PartitionSpec as P

EPS = 1e-06
GELU_A = 0.7978845608028654
GELU_B = 0.044715
CHIPS = ("y", "x")
CAND = ("y", "x", "c")
MIB = 1 << 20
LANES = 128
f32 = jnp.float32
bf16 = jnp.bfloat16


def in_hbm(*values):
    return tuple(pltpu.with_memory_space_constraint(v, pltpu.HBM) for v in values)


def spread(value, axis, size):
    copies = jnp.broadcast_to(value[None], (size, *value.shape))
    return lax.all_to_all(copies, axis, split_axis=0, concat_axis=0, tiled=True)


def score_kernel(
    weight_ref, own_hbm, other_hbm, unit_ref, code_ref, slope_hbm, message_hbm,
    rows_ref, slope_ref, part_ref, message_ref, in_sems, out_sems,
):
    count = own_hbm.shape[0]
    units = weight_ref.shape[0]
    cut = rows_ref.shape[1]
    chunks = 2 * count // cut

    def fetch(n):
        source = own_hbm if n * cut < count else other_hbm
        first = n * cut % count
        return pltpu.make_async_copy(source.at[pl.ds(first, cut), :], rows_ref.at[n], in_sems.at[n])

    def put(n):
        cols = pl.ds(n * cut, cut)
        return pltpu.make_async_copy(slope_ref.at[:, cols], slope_hbm.at[:, cols], out_sems.at[n])

    for n in range(chunks):
        fetch(n).start()
    block = 512
    tiles = [(n, first) for n in range(chunks) for first in range(0, units, block)]

    def product(n, first):
        if first == 0:
            fetch(n).wait()
        return lax.dot_general(
            weight_ref[first : first + block, :],
            rows_ref[n],
            (((1,), (1,)), ((), ())),
            preferred_element_type=f32,
        )

    ahead = product(*tiles[0])
    for at, (n, first) in enumerate(tiles):
        pre = ahead
        if at + 1 < len(tiles):
            ahead = product(*tiles[at + 1])
        here = slice(first, first + block)
        cols = slice(n * cut, (n + 1) * cut)
        half_unit = 0.5 * unit_ref[here, :]
        line = GELU_A * pre
        cube = (GELU_B * (pre * pre)) * line
        inner = line + cube
        tanh = jnp.tanh(inner)
        upper = 1.0 + tanh
        acts = (pre * upper).astype(bf16).astype(f32)
        part = jnp.sum(acts * half_unit, axis=0, keepdims=True)
        part_ref[:, cols] = part if first == 0 else part_ref[:, cols] + part
        slope_ref[here, cols] = half_unit * (
            upper + (1.0 - tanh * tanh) * (inner + (cube + cube))
        )
        if first + block == units:
            put(n).start()
    row = jnp.concatenate([part_ref[...], code_ref[...]], axis=1)
    for d in range(message_ref.shape[0]):
        message_ref[d] = row
    send = pltpu.make_async_copy(message_ref, message_hbm, out_sems.at[chunks])
    send.start()
    for n in range(chunks):
        put(n).wait()
    send.wait()


def score(weight, own, other, unit, code, devices):
    units, width = weight.shape
    count = own.shape[0]
    cut = 256
    chunks = 2 * count // cut
    vmem = pl.BlockSpec(memory_space=pltpu.VMEM)
    hbm = pl.BlockSpec(memory_space=pltpu.HBM)
    return pl.pallas_call(
        score_kernel,
        in_specs=[vmem, hbm, hbm, vmem, vmem],
        out_specs=[hbm, hbm],
        out_shape=[
            pltpu.HBM((units, 2 * count), f32),
            pltpu.HBM((devices, 1, 3 * count), f32),
        ],
        scratch_shapes=[
            pltpu.VMEM((chunks, cut, width), bf16),
            pltpu.VMEM((units, 2 * count), f32),
            pltpu.VMEM((1, 2 * count), f32),
            pltpu.VMEM((devices, 1, 3 * count), f32),
            pltpu.SemaphoreType.DMA((chunks,)),
            pltpu.SemaphoreType.DMA((chunks + 1,)),
        ],
        compiler_params=pltpu.CompilerParams(vmem_limit_bytes=40 * MIB),
        cost_estimate=pl.CostEstimate(
            flops=4 * units * width * count,
            bytes_accessed=12 * MIB,
            transcendentals=2 * units * count,
        ),
        name="score",
    )(weight, *in_hbm(own, other), unit, code)


def term_kernel(
    place_ref, heard_ref, half_ref, slope_hbm, own_hbm, other_hbm, lam_ref, term_ref,
    raw_ref, far_ref, own_ref, sum_ref, slope_ref, rows_ref, sems,
):
    count = own_hbm.shape[0]
    units = slope_hbm.shape[0]
    block = units // 2
    fetches = [
        pltpu.make_async_copy(own_hbm, rows_ref.at[0], sems.at[0]),
        pltpu.make_async_copy(other_hbm, rows_ref.at[1], sems.at[1]),
        pltpu.make_async_copy(slope_hbm, slope_ref, sems.at[2]),
    ]
    for fetch in fetches:
        fetch.start()
    devices, _, size = heard_ref.shape
    width = size // 3
    local = 32
    for d in range(devices):
        raw_ref[d : d + 1, :] = heard_ref[d]
    row = lax.broadcasted_iota(jnp.int32, (devices, width), 0)
    near = raw_ref[:, width : 2 * width]
    near = jnp.where(row % 2 == 0, pltpu.roll(near, devices - 1, 0), pltpu.roll(near, 1, 0))
    code = raw_ref[:, 2 * width :]
    rank = jnp.floor(code * 0.125)
    level = (code - 8.0 * rank).astype(jnp.int32)
    far_ref[0] = 0.5 * (raw_ref[:, :width] + near)
    far_ref[1] = (jnp.left_shift(jnp.ones_like(level), level) - 1).astype(f32)
    far_ref[2] = 0.6931471805599453 / jnp.log(2.0 + rank)

    lane = lax.broadcasted_iota(jnp.int32, (LANES, LANES), 1)
    sub = lax.broadcasted_iota(jnp.int32, (LANES, LANES), 0)
    ones = (lane // local == sub // local).astype(f32)
    pick = lax.broadcasted_iota(jnp.int32, (local, width), 1) % local == lax.broadcasted_iota(
        jnp.int32, (local, width), 0
    )
    for c in range(2):
        mine = row == 2 * place_ref[0] + c
        for k in range(3):
            value = jnp.sum(jnp.where(mine, far_ref[k], 0.0), axis=0, keepdims=True)
            value = jnp.where(pick, value, 0.0)
            for first in range(0, width, LANES):
                at = ((first // LANES * 3 + k) * 2 + c) * local
                own_ref[at : at + local, :] = value[:, first : first + LANES]
    own_ref[...] = jnp.dot(
        own_ref[...], ones, precision=lax.Precision.HIGHEST, preferred_element_type=f32
    )
    pairs = 2 * local
    for first in range(0, width, LANES):
        cols = slice(first, first + LANES)
        at = first // LANES * 3 * pairs
        own_score, own_gain, own_disc = (
            own_ref[at + k * pairs : at + (k + 1) * pairs, :] for k in range(3)
        )

        def step(n, total):
            rows = pl.ds(pl.multiple_of(8 * n, 8), 8)
            score, gain, disc = far_ref[0, rows, cols], far_ref[1, rows, cols], far_ref[2, rows, cols]
            for j in range(8):
                gain_diff = gain[j : j + 1] - own_gain
                disc_diff = jnp.abs(disc[j : j + 1] - own_disc)
                pull = gain_diff * disc_diff
                total += pull + jnp.abs(pull) * jnp.tanh(own_score - score[j : j + 1])
            return total

        at = first // LANES * pairs
        sum_ref[at : at + pairs, :] = lax.fori_loop(0, devices // 8, step, jnp.zeros((pairs, LANES), f32))
    sum_ref[...] = jnp.dot(
        sum_ref[...], ones, precision=lax.Precision.HIGHEST, preferred_element_type=f32
    )
    for first in range(0, width, LANES):
        cols = slice(first, first + LANES)
        at = first // LANES * pairs
        lam = [
            half_ref[:, cols]
            * jnp.sum(
                jnp.where(pick[:, cols], sum_ref[at + c * local : at + (c + 1) * local, :], 0.0), axis=0, keepdims=True
            )
            for c in range(2)
        ]
        south = place_ref[1] == 0
        lam_ref[0:1, cols] = jnp.where(south, lam[0], lam[1])
        lam_ref[1:2, cols] = jnp.where(south, lam[1], lam[0])
    for fetch in fetches:
        fetch.wait()
    for first in range(0, units, block):
        here = slice(first, first + block)
        term = None
        for k in range(2):
            slope = slope_ref[here, k * count : (k + 1) * count]
            grad_pre = (slope * lam_ref[k : k + 1, :]).astype(bf16)
            part = jnp.dot(grad_pre, rows_ref[k], preferred_element_type=f32)
            term = part if term is None else term + part
        term_ref[here, :] = term.astype(bf16)


def gradient_term(heard, half, place, slope, own, other):
    devices, _, size = heard.shape
    units = slope.shape[0]
    count, width = own.shape
    pairs = 64 * (count // LANES)
    vmem = pl.BlockSpec(memory_space=pltpu.VMEM)
    hbm = pl.BlockSpec(memory_space=pltpu.HBM)
    return pl.pallas_call(
        term_kernel,
        in_specs=[pl.BlockSpec(memory_space=pltpu.SMEM), vmem, vmem, hbm, hbm, hbm],
        out_specs=[vmem, vmem],
        out_shape=[
            jax.ShapeDtypeStruct((2, count), f32),
            jax.ShapeDtypeStruct((units, width), bf16),
        ],
        scratch_shapes=[
            pltpu.VMEM((devices, size), f32),
            pltpu.VMEM((3, devices, count), f32),
            pltpu.VMEM((3 * pairs, LANES), f32),
            pltpu.VMEM((pairs, LANES), f32),
            pltpu.VMEM(slope.shape, f32),
            pltpu.VMEM((2, count, width), bf16),
            pltpu.SemaphoreType.DMA((3,)),
        ],
        compiler_params=pltpu.CompilerParams(vmem_limit_bytes=40 * MIB),
        cost_estimate=pl.CostEstimate(
            flops=4 * units * width * count, bytes_accessed=12 * MIB, transcendentals=2 * MIB
        ),
        name="gradient_term",
    )(place, heard, half, *in_hbm(slope, own, other))


def copies_kernel(block_hbm, out_hbm, block_ref, in_sems, out_sems):
    count, parts = out_hbm.shape[0], in_sems.shape[0]
    size = block_hbm.shape[0] // parts
    cuts = [pl.ds(n * size, size) for n in range(parts)]
    fetches = [
        pltpu.make_async_copy(block_hbm.at[cut, :], block_ref.at[cut, :], in_sems.at[n])
        for n, cut in enumerate(cuts)
    ]
    for fetch in fetches:
        fetch.start()
    puts = []
    for n, cut in enumerate(cuts):
        fetches[n].wait()
        for k in range(count):
            put = pltpu.make_async_copy(
                block_ref.at[cut, :], out_hbm.at[k, cut, :], out_sems.at[n * count + k]
            )
            put.start()
            puts.append(put)
    for put in puts:
        put.wait()


def copies(block, count):
    hbm = pl.BlockSpec(memory_space=pltpu.HBM)
    return pl.pallas_call(
        copies_kernel,
        in_specs=[hbm],
        out_specs=hbm,
        out_shape=pltpu.HBM((count, *block.shape), block.dtype),
        scratch_shapes=[
            pltpu.VMEM(block.shape, block.dtype),
            pltpu.SemaphoreType.DMA((2,)),
            pltpu.SemaphoreType.DMA((2 * count,)),
        ],
        compiler_params=pltpu.CompilerParams(vmem_limit_bytes=16 * MIB),
        name="copies",
    )(*in_hbm(block))


def squares_kernel(total_ref, out_ref):
    total = total_ref[...].astype(f32)
    square = jnp.sum(total * total, axis=0)
    square = jnp.sum(jnp.sum(square, axis=0, keepdims=True), axis=1, keepdims=True)
    row = jnp.broadcast_to(square, (1, LANES))
    for d in range(out_ref.shape[0]):
        out_ref[d] = row


def squares(total, devices):
    return pl.pallas_call(
        squares_kernel,
        in_specs=[pl.BlockSpec(memory_space=pltpu.VMEM)],
        out_specs=pl.BlockSpec(memory_space=pltpu.VMEM),
        out_shape=jax.ShapeDtypeStruct((devices, 1, LANES), f32),
        compiler_params=pltpu.CompilerParams(vmem_limit_bytes=16 * MIB),
        name="squares",
    )(total)


def scaled_kernel(entries, total_ref, heard_ref, out_ref):
    square = jnp.sum(heard_ref[...], axis=0)
    scale = lax.rsqrt(square * (1.0 / entries) + EPS)
    planes, rows, cut = total_ref.shape
    across = out_ref.shape[1] // cut
    scale = jnp.concatenate([scale] * (cut // LANES), axis=1)
    for k in range(planes):
        at, col = k // across * rows, k % across * cut
        out_ref[at : at + rows, col : col + cut] = total_ref[k].astype(f32) * scale


def scaled(total, heard, rows, width, entries):
    return pl.pallas_call(
        functools.partial(scaled_kernel, entries),
        in_specs=[pl.BlockSpec(memory_space=pltpu.VMEM)] * 2,
        out_specs=pl.BlockSpec(memory_space=pltpu.VMEM),
        out_shape=jax.ShapeDtypeStruct((rows, width), f32),
        compiler_params=pltpu.CompilerParams(vmem_limit_bytes=16 * MIB),
        name="scaled",
    )(total, heard)


def per_device(embeddings, hidden_weight, score_weight, relevance, rank_pos, ideal_dcg):
    groups, local, width = embeddings.shape
    owned_rows = hidden_weight.shape[0]
    cores = lax.axis_size("c")
    chips = lax.axis_size("y") * lax.axis_size("x")
    planes = lax.axis_size("z")
    core = lax.axis_index("c")
    chip = lax.axis_index("y") * lax.axis_size("x") + lax.axis_index("x")
    own = embeddings.reshape(groups * local, width)

    weight = lax.all_to_all(
        copies(hidden_weight, chips), CHIPS, split_axis=0, concat_axis=0, tiled=True
    ).reshape(chips * owned_rows, width)
    other = lax.ppermute(own, "c", [(0, 1), (1, 0)])
    unit = lax.dynamic_index_in_dim(
        score_weight.reshape(chips, cores, owned_rows), core, 1, keepdims=False
    ).reshape(chips * owned_rows, 1).astype(f32)
    code = (8 * rank_pos + relevance).astype(f32).reshape(1, groups * local)
    half = jnp.repeat(0.5 / ideal_dcg, local).reshape(1, groups * local)
    place = jnp.stack([chip, core]).astype(jnp.int32)

    slope, message = score(weight, own, other, unit, code, chips * cores)
    heard = lax.all_to_all(message, CAND, split_axis=0, concat_axis=0, tiled=True)
    lam, term = gradient_term(heard, half, place, slope, own, other)
    lambdas = lam[0].reshape(groups, local)
    terms = lax.all_to_all(
        term.reshape(chips, owned_rows, width), CHIPS, split_axis=0, concat_axis=0, tiled=True
    )
    owned = jnp.sum(terms.astype(f32), axis=0).astype(bf16)
    across = planes * 8 // owned_rows
    owned = owned.reshape(owned_rows // 8, 8, across, width // across).transpose(0, 2, 1, 3)
    pieces = lax.all_to_all(
        owned.reshape(planes, 8, width // across), "z", split_axis=0, concat_axis=0, tiled=True
    )
    piece = jnp.sum(pieces.astype(f32), axis=0).astype(bf16)
    total = spread(piece, "z", planes)
    entries = owned_rows * width * chips * cores
    square = lax.all_to_all(
        squares(total, chips * cores), CAND, split_axis=0, concat_axis=0, tiled=True
    )
    return scaled(total, square, owned_rows, width, entries), lambdas


def solution(mesh):
    fine = Mesh(mesh.devices.reshape(mesh.devices.shape[0], 4, 4, 2), ("z", "y", "x", "c"))
    return jax.shard_map(
        per_device,
        mesh=fine,
        in_specs=(
            P("z", CAND, None),
            P(CAND, None),
            P(),
            P("z", CAND),
            P("z", CAND),
            P("z"),
        ),
        out_specs=(P(CAND, None), P("z", CAND)),
        check_vma=False,
    )
```

```python
import functools

import jax
import jax.numpy as jnp
from jax import lax
from jax.experimental import pallas as pl
from jax.experimental.pallas import tpu as pltpu
from jax.sharding import Mesh
from jax.sharding import PartitionSpec as P

EPS = 1e-06
GELU_A = 0.7978845608028654
GELU_B = 0.044715
CHIPS = ("x", "y")
CAND = ("y", "x", "c")
MIB = 1 << 20
LANES = 128
f32 = jnp.float32
bf16 = jnp.bfloat16


def in_hbm(*values):
    return tuple(pltpu.with_memory_space_constraint(v, pltpu.HBM) for v in values)


def spread(value, axis, size):
    copies = jnp.broadcast_to(value[None], (size, *value.shape))
    return lax.all_to_all(copies, axis, split_axis=0, concat_axis=0, tiled=True)


def score_kernel(
    weight_ref, own_hbm, other_hbm, unit_ref, code_ref, slope_hbm, message_hbm,
    rows_ref, slope_ref, part_ref, message_ref, in_sems, out_sems,
):
    count = own_hbm.shape[0]
    units = weight_ref.shape[0]
    cut = rows_ref.shape[1]
    chunks = 2 * count // cut

    def fetch(n):
        source = own_hbm if n * cut < count else other_hbm
        first = n * cut % count
        return pltpu.make_async_copy(source.at[pl.ds(first, cut), :], rows_ref.at[n], in_sems.at[n])

    def put(n):
        cols = pl.ds(n * cut, cut)
        return pltpu.make_async_copy(slope_ref.at[:, cols], slope_hbm.at[:, cols], out_sems.at[n])

    for n in range(chunks):
        fetch(n).start()
    block = 512
    tiles = [(n, first) for n in range(chunks) for first in range(0, units, block)]

    def product(n, first):
        if first == 0:
            fetch(n).wait()
        return lax.dot_general(
            weight_ref[first : first + block, :],
            rows_ref[n],
            (((1,), (1,)), ((), ())),
            preferred_element_type=f32,
        )

    ahead = product(*tiles[0])
    for at, (n, first) in enumerate(tiles):
        pre = ahead
        if at + 1 < len(tiles):
            ahead = product(*tiles[at + 1])
        here = slice(first, first + block)
        cols = slice(n * cut, (n + 1) * cut)
        half_unit = 0.5 * unit_ref[here, :]
        line = GELU_A * pre
        cube = (GELU_B * (pre * pre)) * line
        inner = line + cube
        tanh = jnp.tanh(inner)
        upper = 1.0 + tanh
        acts = (pre * upper).astype(bf16).astype(f32)
        part = jnp.sum(acts * half_unit, axis=0, keepdims=True)
        part_ref[:, cols] = part if first == 0 else part_ref[:, cols] + part
        slope_ref[here, cols] = half_unit * (
            upper + (1.0 - tanh * tanh) * (inner + (cube + cube))
        )
        if first + block == units:
            put(n).start()
    row = jnp.concatenate([part_ref[...], code_ref[...]], axis=1)
    for d in range(message_ref.shape[0]):
        message_ref[d] = row
    send = pltpu.make_async_copy(message_ref, message_hbm, out_sems.at[chunks])
    send.start()
    for n in range(chunks):
        put(n).wait()
    send.wait()


def score(weight, own, other, unit, code, devices):
    units, width = weight.shape
    count = own.shape[0]
    cut = 256
    chunks = 2 * count // cut
    vmem = pl.BlockSpec(memory_space=pltpu.VMEM)
    hbm = pl.BlockSpec(memory_space=pltpu.HBM)
    return pl.pallas_call(
        score_kernel,
        in_specs=[vmem, hbm, hbm, vmem, vmem],
        out_specs=[hbm, hbm],
        out_shape=[
            pltpu.HBM((units, 2 * count), f32),
            pltpu.HBM((devices, 1, 3 * count), f32),
        ],
        scratch_shapes=[
            pltpu.VMEM((chunks, cut, width), bf16),
            pltpu.VMEM((units, 2 * count), f32),
            pltpu.VMEM((1, 2 * count), f32),
            pltpu.VMEM((devices, 1, 3 * count), f32),
            pltpu.SemaphoreType.DMA((chunks,)),
            pltpu.SemaphoreType.DMA((chunks + 1,)),
        ],
        compiler_params=pltpu.CompilerParams(vmem_limit_bytes=40 * MIB),
        cost_estimate=pl.CostEstimate(
            flops=4 * units * width * count,
            bytes_accessed=12 * MIB,
            transcendentals=2 * units * count,
        ),
        name="score",
    )(weight, *in_hbm(own, other), unit, code)


def term_kernel(
    place_ref, heard_ref, half_ref, slope_hbm, own_hbm, other_hbm, lam_ref, term_ref,
    raw_ref, far_ref, own_ref, sum_ref, slope_ref, rows_ref, sems,
):
    count = own_hbm.shape[0]
    units = slope_hbm.shape[0]
    block = units // 2
    fetches = [
        pltpu.make_async_copy(own_hbm, rows_ref.at[0], sems.at[0]),
        pltpu.make_async_copy(other_hbm, rows_ref.at[1], sems.at[1]),
        pltpu.make_async_copy(slope_hbm, slope_ref, sems.at[2]),
    ]
    for fetch in fetches:
        fetch.start()
    devices, _, size = heard_ref.shape
    width = size // 3
    local = 32
    for d in range(devices):
        raw_ref[d : d + 1, :] = heard_ref[d]
    row = lax.broadcasted_iota(jnp.int32, (devices, width), 0)
    near = raw_ref[:, width : 2 * width]
    near = jnp.where(row % 2 == 0, pltpu.roll(near, devices - 1, 0), pltpu.roll(near, 1, 0))
    code = raw_ref[:, 2 * width :]
    rank = jnp.floor(code * 0.125)
    level = (code - 8.0 * rank).astype(jnp.int32)
    far_ref[0] = 0.5 * (raw_ref[:, :width] + near)
    far_ref[1] = (jnp.left_shift(jnp.ones_like(level), level) - 1).astype(f32)
    far_ref[2] = 0.6931471805599453 / jnp.log(2.0 + rank)

    lane = lax.broadcasted_iota(jnp.int32, (LANES, LANES), 1)
    sub = lax.broadcasted_iota(jnp.int32, (LANES, LANES), 0)
    ones = (lane // local == sub // local).astype(f32)
    pick = lax.broadcasted_iota(jnp.int32, (local, width), 1) % local == lax.broadcasted_iota(
        jnp.int32, (local, width), 0
    )
    for c in range(2):
        mine = row == 2 * place_ref[0] + c
        for k in range(3):
            value = jnp.sum(jnp.where(mine, far_ref[k], 0.0), axis=0, keepdims=True)
            value = jnp.where(pick, value, 0.0)
            for first in range(0, width, LANES):
                at = ((first // LANES * 3 + k) * 2 + c) * local
                own_ref[at : at + local, :] = value[:, first : first + LANES]
    own_ref[...] = jnp.dot(
        own_ref[...], ones, precision=lax.Precision.HIGHEST, preferred_element_type=f32
    )
    pairs = 2 * local
    for first in range(0, width, LANES):
        cols = slice(first, first + LANES)
        at = first // LANES * 3 * pairs
        own_score, own_gain, own_disc = (
            own_ref[at + k * pairs : at + (k + 1) * pairs, :] for k in range(3)
        )

        def step(n, total):
            rows = pl.ds(pl.multiple_of(8 * n, 8), 8)
            score, gain, disc = far_ref[0, rows, cols], far_ref[1, rows, cols], far_ref[2, rows, cols]
            for j in range(8):
                gain_diff = gain[j : j + 1] - own_gain
                disc_diff = jnp.abs(disc[j : j + 1] - own_disc)
                pull = gain_diff * disc_diff
                total += pull + jnp.abs(pull) * jnp.tanh(own_score - score[j : j + 1])
            return total

        at = first // LANES * pairs
        sum_ref[at : at + pairs, :] = lax.fori_loop(0, devices // 8, step, jnp.zeros((pairs, LANES), f32))
    sum_ref[...] = jnp.dot(
        sum_ref[...], ones, precision=lax.Precision.HIGHEST, preferred_element_type=f32
    )
    for first in range(0, width, LANES):
        cols = slice(first, first + LANES)
        at = first // LANES * pairs
        lam = [
            half_ref[:, cols]
            * jnp.sum(
                jnp.where(pick[:, cols], sum_ref[at + c * local : at + (c + 1) * local, :], 0.0), axis=0, keepdims=True
            )
            for c in range(2)
        ]
        south = place_ref[1] == 0
        lam_ref[0:1, cols] = jnp.where(south, lam[0], lam[1])
        lam_ref[1:2, cols] = jnp.where(south, lam[1], lam[0])
    for fetch in fetches:
        fetch.wait()
    for first in range(0, units, block):
        here = slice(first, first + block)
        term = None
        for k in range(2):
            slope = slope_ref[here, k * count : (k + 1) * count]
            grad_pre = (slope * lam_ref[k : k + 1, :]).astype(bf16)
            part = jnp.dot(grad_pre, rows_ref[k], preferred_element_type=f32)
            term = part if term is None else term + part
        term_ref[here, :] = term.astype(bf16)


def gradient_term(heard, half, place, slope, own, other):
    devices, _, size = heard.shape
    units = slope.shape[0]
    count, width = own.shape
    pairs = 64 * (count // LANES)
    vmem = pl.BlockSpec(memory_space=pltpu.VMEM)
    hbm = pl.BlockSpec(memory_space=pltpu.HBM)
    return pl.pallas_call(
        term_kernel,
        in_specs=[pl.BlockSpec(memory_space=pltpu.SMEM), vmem, vmem, hbm, hbm, hbm],
        out_specs=[vmem, vmem],
        out_shape=[
            jax.ShapeDtypeStruct((2, count), f32),
            jax.ShapeDtypeStruct((units, width), bf16),
        ],
        scratch_shapes=[
            pltpu.VMEM((devices, size), f32),
            pltpu.VMEM((3, devices, count), f32),
            pltpu.VMEM((3 * pairs, LANES), f32),
            pltpu.VMEM((pairs, LANES), f32),
            pltpu.VMEM(slope.shape, f32),
            pltpu.VMEM((2, count, width), bf16),
            pltpu.SemaphoreType.DMA((3,)),
        ],
        compiler_params=pltpu.CompilerParams(vmem_limit_bytes=40 * MIB),
        cost_estimate=pl.CostEstimate(
            flops=4 * units * width * count, bytes_accessed=12 * MIB, transcendentals=2 * MIB
        ),
        name="gradient_term",
    )(place, heard, half, *in_hbm(slope, own, other))


def copies_kernel(block_hbm, out_hbm, block_ref, in_sems, out_sems):
    count, parts = out_hbm.shape[0], in_sems.shape[0]
    size = block_hbm.shape[0] // parts
    cuts = [pl.ds(n * size, size) for n in range(parts)]
    fetches = [
        pltpu.make_async_copy(block_hbm.at[cut, :], block_ref.at[cut, :], in_sems.at[n])
        for n, cut in enumerate(cuts)
    ]
    for fetch in fetches:
        fetch.start()
    puts = []
    for n, cut in enumerate(cuts):
        fetches[n].wait()
        for k in range(count):
            put = pltpu.make_async_copy(
                block_ref.at[cut, :], out_hbm.at[k, cut, :], out_sems.at[n * count + k]
            )
            put.start()
            puts.append(put)
    for put in puts:
        put.wait()


def copies(block, count):
    hbm = pl.BlockSpec(memory_space=pltpu.HBM)
    return pl.pallas_call(
        copies_kernel,
        in_specs=[hbm],
        out_specs=hbm,
        out_shape=pltpu.HBM((count, *block.shape), block.dtype),
        scratch_shapes=[
            pltpu.VMEM(block.shape, block.dtype),
            pltpu.SemaphoreType.DMA((2,)),
            pltpu.SemaphoreType.DMA((2 * count,)),
        ],
        compiler_params=pltpu.CompilerParams(vmem_limit_bytes=16 * MIB),
        name="copies",
    )(*in_hbm(block))


def squares_kernel(total_ref, out_ref):
    total = total_ref[...].astype(f32)
    square = jnp.sum(total * total, axis=0)
    square = jnp.sum(jnp.sum(square, axis=0, keepdims=True), axis=1, keepdims=True)
    row = jnp.broadcast_to(square, (1, LANES))
    for d in range(out_ref.shape[0]):
        out_ref[d] = row


def squares(total, devices):
    return pl.pallas_call(
        squares_kernel,
        in_specs=[pl.BlockSpec(memory_space=pltpu.VMEM)],
        out_specs=pl.BlockSpec(memory_space=pltpu.VMEM),
        out_shape=jax.ShapeDtypeStruct((devices, 1, LANES), f32),
        compiler_params=pltpu.CompilerParams(vmem_limit_bytes=16 * MIB),
        name="squares",
    )(total)


def scaled_kernel(entries, total_ref, heard_ref, out_ref):
    square = jnp.sum(heard_ref[...], axis=0)
    scale = lax.rsqrt(square * (1.0 / entries) + EPS)
    planes, rows, cut = total_ref.shape
    across = out_ref.shape[1] // cut
    scale = jnp.concatenate([scale] * (cut // LANES), axis=1)
    for k in range(planes):
        at, col = k // across * rows, k % across * cut
        out_ref[at : at + rows, col : col + cut] = total_ref[k].astype(f32) * scale


def scaled(total, heard, rows, width, entries):
    return pl.pallas_call(
        functools.partial(scaled_kernel, entries),
        in_specs=[pl.BlockSpec(memory_space=pltpu.VMEM)] * 2,
        out_specs=pl.BlockSpec(memory_space=pltpu.VMEM),
        out_shape=jax.ShapeDtypeStruct((rows, width), f32),
        compiler_params=pltpu.CompilerParams(vmem_limit_bytes=16 * MIB),
        name="scaled",
    )(total, heard)


def per_device(embeddings, hidden_weight, score_weight, relevance, rank_pos, ideal_dcg):
    groups, local, width = embeddings.shape
    owned_rows = hidden_weight.shape[0]
    cores = lax.axis_size("c")
    chips = lax.axis_size("y") * lax.axis_size("x")
    planes = lax.axis_size("z")
    core = lax.axis_index("c")
    chip = lax.axis_index("y") * lax.axis_size("x") + lax.axis_index("x")
    own = embeddings.reshape(groups * local, width)

    weight = lax.all_to_all(
        copies(hidden_weight, chips), CHIPS, split_axis=0, concat_axis=0, tiled=True
    ).reshape(chips * owned_rows, width)
    other = lax.ppermute(own, "c", [(0, 1), (1, 0)])
    unit = lax.dynamic_index_in_dim(
        score_weight.reshape(
            lax.axis_size("y"), lax.axis_size("x"), cores, owned_rows
        ).transpose(1, 0, 2, 3),
        core,
        2,
        keepdims=False,
    ).reshape(chips * owned_rows, 1).astype(f32)
    code = (8 * rank_pos + relevance).astype(f32).reshape(1, groups * local)
    half = jnp.repeat(0.5 / ideal_dcg, local).reshape(1, groups * local)
    place = jnp.stack([chip, core]).astype(jnp.int32)

    slope, message = score(weight, own, other, unit, code, chips * cores)
    heard = lax.all_to_all(message, CAND, split_axis=0, concat_axis=0, tiled=True)
    lam, term = gradient_term(heard, half, place, slope, own, other)
    lambdas = lam[0].reshape(groups, local)
    terms = lax.all_to_all(
        term.reshape(chips, owned_rows, width), CHIPS, split_axis=0, concat_axis=0, tiled=True
    )
    owned = jnp.sum(terms.astype(f32), axis=0).astype(bf16)
    across = planes * 8 // owned_rows
    owned = owned.reshape(owned_rows // 8, 8, across, width // across).transpose(0, 2, 1, 3)
    pieces = lax.all_to_all(
        owned.reshape(planes, 8, width // across), "z", split_axis=0, concat_axis=0, tiled=True
    )
    piece = jnp.sum(pieces.astype(f32), axis=0).astype(bf16)
    total = spread(piece, "z", planes)
    entries = owned_rows * width * chips * cores
    square = lax.all_to_all(
        squares(total, chips * cores), CAND, split_axis=0, concat_axis=0, tiled=True
    )
    return scaled(total, square, owned_rows, width, entries), lambdas


def solution(mesh):
    fine = Mesh(mesh.devices.reshape(mesh.devices.shape[0], 4, 4, 2), ("z", "y", "x", "c"))
    return jax.shard_map(
        per_device,
        mesh=fine,
        in_specs=(
            P("z", CAND, None),
            P(CAND, None),
            P(),
            P("z", CAND),
            P("z", CAND),
            P("z"),
        ),
        out_specs=(P(CAND, None), P("z", CAND)),
        check_vma=False,
    )
```

```python
import functools

import jax
import jax.numpy as jnp
from jax import lax
from jax.experimental import pallas as pl
from jax.experimental.pallas import tpu as pltpu
from jax.sharding import Mesh
from jax.sharding import PartitionSpec as P

EPS = 1e-06
GELU_A = 0.7978845608028654
GELU_B = 0.044715
CHIPS = ("x", "y")
CAND = ("y", "x", "c")
EVERY = ("x", "y", "c")
MIB = 1 << 20
LANES = 128
f32 = jnp.float32
bf16 = jnp.bfloat16


def in_hbm(*values):
    return tuple(pltpu.with_memory_space_constraint(v, pltpu.HBM) for v in values)


def spread(value, axis, size):
    copies = jnp.broadcast_to(value[None], (size, *value.shape))
    return lax.all_to_all(copies, axis, split_axis=0, concat_axis=0, tiled=True)


def score_kernel(
    weight_ref, own_hbm, other_hbm, unit_ref, code_ref, slope_hbm, message_hbm,
    rows_ref, slope_ref, part_ref, message_ref, in_sems, out_sems,
):
    count = own_hbm.shape[0]
    units = weight_ref.shape[0]
    cut = rows_ref.shape[1]
    chunks = 2 * count // cut

    def fetch(n):
        source = own_hbm if n * cut < count else other_hbm
        first = n * cut % count
        return pltpu.make_async_copy(source.at[pl.ds(first, cut), :], rows_ref.at[n], in_sems.at[n])

    def put(n):
        cols = pl.ds(n * cut, cut)
        return pltpu.make_async_copy(slope_ref.at[:, cols], slope_hbm.at[:, cols], out_sems.at[n])

    for n in range(chunks):
        fetch(n).start()
    block = 512
    tiles = [(n, first) for n in range(chunks) for first in range(0, units, block)]

    def product(n, first):
        if first == 0:
            fetch(n).wait()
        return lax.dot_general(
            weight_ref[first : first + block, :],
            rows_ref[n],
            (((1,), (1,)), ((), ())),
            preferred_element_type=f32,
        )

    ahead = product(*tiles[0])
    for at, (n, first) in enumerate(tiles):
        pre = ahead
        if at + 1 < len(tiles):
            ahead = product(*tiles[at + 1])
        here = slice(first, first + block)
        cols = slice(n * cut, (n + 1) * cut)
        half_unit = 0.5 * unit_ref[here, :]
        line = GELU_A * pre
        cube = (GELU_B * (pre * pre)) * line
        inner = line + cube
        tanh = jnp.tanh(inner)
        upper = 1.0 + tanh
        acts = (pre * upper).astype(bf16).astype(f32)
        part = jnp.sum(acts * half_unit, axis=0, keepdims=True)
        part_ref[:, cols] = part if first == 0 else part_ref[:, cols] + part
        slope_ref[here, cols] = half_unit * (
            upper + (1.0 - tanh * tanh) * (inner + (cube + cube))
        )
        if first + block == units:
            put(n).start()
    row = jnp.concatenate([part_ref[...], code_ref[...]], axis=1)
    for d in range(message_ref.shape[0]):
        message_ref[d] = row
    send = pltpu.make_async_copy(message_ref, message_hbm, out_sems.at[chunks])
    send.start()
    for n in range(chunks):
        put(n).wait()
    send.wait()


def score(weight, own, other, unit, code, devices):
    units, width = weight.shape
    count = own.shape[0]
    cut = 256
    chunks = 2 * count // cut
    vmem = pl.BlockSpec(memory_space=pltpu.VMEM)
    hbm = pl.BlockSpec(memory_space=pltpu.HBM)
    return pl.pallas_call(
        score_kernel,
        in_specs=[vmem, hbm, hbm, vmem, vmem],
        out_specs=[hbm, hbm],
        out_shape=[
            pltpu.HBM((units, 2 * count), f32),
            pltpu.HBM((devices, 1, 3 * count), f32),
        ],
        scratch_shapes=[
            pltpu.VMEM((chunks, cut, width), bf16),
            pltpu.VMEM((units, 2 * count), f32),
            pltpu.VMEM((1, 2 * count), f32),
            pltpu.VMEM((devices, 1, 3 * count), f32),
            pltpu.SemaphoreType.DMA((chunks,)),
            pltpu.SemaphoreType.DMA((chunks + 1,)),
        ],
        compiler_params=pltpu.CompilerParams(vmem_limit_bytes=40 * MIB),
        cost_estimate=pl.CostEstimate(
            flops=4 * units * width * count,
            bytes_accessed=12 * MIB,
            transcendentals=2 * units * count,
        ),
        name="score",
    )(weight, *in_hbm(own, other), unit, code)


def term_kernel(
    place_ref, heard_ref, half_ref, slope_hbm, own_hbm, other_hbm, lam_ref, term_ref,
    raw_ref, far_ref, own_ref, sum_ref, slope_ref, rows_ref, sems,
):
    count = own_hbm.shape[0]
    units = slope_hbm.shape[0]
    block = units // 2
    fetches = [
        pltpu.make_async_copy(own_hbm, rows_ref.at[0], sems.at[0]),
        pltpu.make_async_copy(other_hbm, rows_ref.at[1], sems.at[1]),
        pltpu.make_async_copy(slope_hbm, slope_ref, sems.at[2]),
    ]
    for fetch in fetches:
        fetch.start()
    devices, _, size = heard_ref.shape
    width = size // 3
    local = 32
    for d in range(devices):
        raw_ref[d : d + 1, :] = heard_ref[d]
    row = lax.broadcasted_iota(jnp.int32, (devices, width), 0)
    near = raw_ref[:, width : 2 * width]
    near = jnp.where(row % 2 == 0, pltpu.roll(near, devices - 1, 0), pltpu.roll(near, 1, 0))
    code = raw_ref[:, 2 * width :]
    rank = jnp.floor(code * 0.125)
    level = (code - 8.0 * rank).astype(jnp.int32)
    far_ref[0] = 0.5 * (raw_ref[:, :width] + near)
    far_ref[1] = (jnp.left_shift(jnp.ones_like(level), level) - 1).astype(f32)
    far_ref[2] = 0.6931471805599453 / jnp.log(2.0 + rank)

    lane = lax.broadcasted_iota(jnp.int32, (LANES, LANES), 1)
    sub = lax.broadcasted_iota(jnp.int32, (LANES, LANES), 0)
    ones = (lane // local == sub // local).astype(f32)
    pick = lax.broadcasted_iota(jnp.int32, (local, width), 1) % local == lax.broadcasted_iota(
        jnp.int32, (local, width), 0
    )
    for c in range(2):
        mine = row == 2 * place_ref[0] + c
        for k in range(3):
            value = jnp.sum(jnp.where(mine, far_ref[k], 0.0), axis=0, keepdims=True)
            value = jnp.where(pick, value, 0.0)
            for first in range(0, width, LANES):
                at = ((first // LANES * 3 + k) * 2 + c) * local
                own_ref[at : at + local, :] = value[:, first : first + LANES]
    own_ref[...] = jnp.dot(
        own_ref[...], ones, precision=lax.Precision.HIGHEST, preferred_element_type=f32
    )
    pairs = 2 * local
    for first in range(0, width, LANES):
        cols = slice(first, first + LANES)
        at = first // LANES * 3 * pairs
        own_score, own_gain, own_disc = (
            own_ref[at + k * pairs : at + (k + 1) * pairs, :] for k in range(3)
        )

        def step(n, total):
            rows = pl.ds(pl.multiple_of(8 * n, 8), 8)
            score, gain, disc = far_ref[0, rows, cols], far_ref[1, rows, cols], far_ref[2, rows, cols]
            for j in range(8):
                gain_diff = gain[j : j + 1] - own_gain
                disc_diff = jnp.abs(disc[j : j + 1] - own_disc)
                pull = gain_diff * disc_diff
                total += pull + jnp.abs(pull) * jnp.tanh(own_score - score[j : j + 1])
            return total

        at = first // LANES * pairs
        sum_ref[at : at + pairs, :] = lax.fori_loop(0, devices // 8, step, jnp.zeros((pairs, LANES), f32))
    sum_ref[...] = jnp.dot(
        sum_ref[...], ones, precision=lax.Precision.HIGHEST, preferred_element_type=f32
    )
    for first in range(0, width, LANES):
        cols = slice(first, first + LANES)
        at = first // LANES * pairs
        lam = [
            half_ref[:, cols]
            * jnp.sum(
                jnp.where(pick[:, cols], sum_ref[at + c * local : at + (c + 1) * local, :], 0.0), axis=0, keepdims=True
            )
            for c in range(2)
        ]
        south = place_ref[1] == 0
        lam_ref[0:1, cols] = jnp.where(south, lam[0], lam[1])
        lam_ref[1:2, cols] = jnp.where(south, lam[1], lam[0])
    for fetch in fetches:
        fetch.wait()
    for first in range(0, units, block):
        here = slice(first, first + block)
        term = None
        for k in range(2):
            slope = slope_ref[here, k * count : (k + 1) * count]
            grad_pre = (slope * lam_ref[k : k + 1, :]).astype(bf16)
            part = jnp.dot(grad_pre, rows_ref[k], preferred_element_type=f32)
            term = part if term is None else term + part
        term_ref[here, :] = term.astype(bf16)


def gradient_term(heard, half, place, slope, own, other):
    devices, _, size = heard.shape
    units = slope.shape[0]
    count, width = own.shape
    pairs = 64 * (count // LANES)
    vmem = pl.BlockSpec(memory_space=pltpu.VMEM)
    hbm = pl.BlockSpec(memory_space=pltpu.HBM)
    return pl.pallas_call(
        term_kernel,
        in_specs=[pl.BlockSpec(memory_space=pltpu.SMEM), vmem, vmem, hbm, hbm, hbm],
        out_specs=[vmem, vmem],
        out_shape=[
            jax.ShapeDtypeStruct((2, count), f32),
            jax.ShapeDtypeStruct((units, width), bf16),
        ],
        scratch_shapes=[
            pltpu.VMEM((devices, size), f32),
            pltpu.VMEM((3, devices, count), f32),
            pltpu.VMEM((3 * pairs, LANES), f32),
            pltpu.VMEM((pairs, LANES), f32),
            pltpu.VMEM(slope.shape, f32),
            pltpu.VMEM((2, count, width), bf16),
            pltpu.SemaphoreType.DMA((3,)),
        ],
        compiler_params=pltpu.CompilerParams(vmem_limit_bytes=40 * MIB),
        cost_estimate=pl.CostEstimate(
            flops=4 * units * width * count, bytes_accessed=12 * MIB, transcendentals=2 * MIB
        ),
        name="gradient_term",
    )(place, heard, half, *in_hbm(slope, own, other))


def copies_kernel(block_hbm, out_hbm, block_ref, in_sems, out_sems):
    count, parts = out_hbm.shape[0], in_sems.shape[0]
    size = block_hbm.shape[0] // parts
    cuts = [pl.ds(n * size, size) for n in range(parts)]
    fetches = [
        pltpu.make_async_copy(block_hbm.at[cut, :], block_ref.at[cut, :], in_sems.at[n])
        for n, cut in enumerate(cuts)
    ]
    for fetch in fetches:
        fetch.start()
    puts = []
    for n, cut in enumerate(cuts):
        fetches[n].wait()
        for k in range(count):
            put = pltpu.make_async_copy(
                block_ref.at[cut, :], out_hbm.at[k, cut, :], out_sems.at[n * count + k]
            )
            put.start()
            puts.append(put)
    for put in puts:
        put.wait()


def copies(block, count):
    hbm = pl.BlockSpec(memory_space=pltpu.HBM)
    return pl.pallas_call(
        copies_kernel,
        in_specs=[hbm],
        out_specs=hbm,
        out_shape=pltpu.HBM((count, *block.shape), block.dtype),
        scratch_shapes=[
            pltpu.VMEM(block.shape, block.dtype),
            pltpu.SemaphoreType.DMA((2,)),
            pltpu.SemaphoreType.DMA((2 * count,)),
        ],
        compiler_params=pltpu.CompilerParams(vmem_limit_bytes=16 * MIB),
        name="copies",
    )(*in_hbm(block))


def squares_kernel(total_ref, out_ref):
    total = total_ref[...].astype(f32)
    square = jnp.sum(total * total, axis=0)
    square = jnp.sum(jnp.sum(square, axis=0, keepdims=True), axis=1, keepdims=True)
    row = jnp.broadcast_to(square, (1, LANES))
    for d in range(out_ref.shape[0]):
        out_ref[d] = row


def squares(total, devices):
    return pl.pallas_call(
        squares_kernel,
        in_specs=[pl.BlockSpec(memory_space=pltpu.VMEM)],
        out_specs=pl.BlockSpec(memory_space=pltpu.VMEM),
        out_shape=jax.ShapeDtypeStruct((devices, 1, LANES), f32),
        compiler_params=pltpu.CompilerParams(vmem_limit_bytes=16 * MIB),
        name="squares",
    )(total)


def scaled_kernel(entries, total_ref, heard_ref, out_ref):
    square = jnp.sum(heard_ref[...], axis=0)
    scale = lax.rsqrt(square * (1.0 / entries) + EPS)
    planes, rows, cut = total_ref.shape
    across = out_ref.shape[1] // cut
    scale = jnp.concatenate([scale] * (cut // LANES), axis=1)
    for k in range(planes):
        at, col = k // across * rows, k % across * cut
        out_ref[at : at + rows, col : col + cut] = total_ref[k].astype(f32) * scale


def scaled(total, heard, rows, width, entries):
    return pl.pallas_call(
        functools.partial(scaled_kernel, entries),
        in_specs=[pl.BlockSpec(memory_space=pltpu.VMEM)] * 2,
        out_specs=pl.BlockSpec(memory_space=pltpu.VMEM),
        out_shape=jax.ShapeDtypeStruct((rows, width), f32),
        compiler_params=pltpu.CompilerParams(vmem_limit_bytes=16 * MIB),
        name="scaled",
    )(total, heard)


def per_device(embeddings, hidden_weight, score_weight, relevance, rank_pos, ideal_dcg):
    groups, local, width = embeddings.shape
    owned_rows = hidden_weight.shape[0]
    cores = lax.axis_size("c")
    chips = lax.axis_size("y") * lax.axis_size("x")
    planes = lax.axis_size("z")
    core = lax.axis_index("c")
    chip = lax.axis_index("x") * lax.axis_size("y") + lax.axis_index("y")
    own = embeddings.reshape(groups * local, width)

    weight = lax.all_to_all(
        copies(hidden_weight, chips), CHIPS, split_axis=0, concat_axis=0, tiled=True
    ).reshape(chips * owned_rows, width)
    other = lax.ppermute(own, "c", [(0, 1), (1, 0)])
    unit = lax.dynamic_index_in_dim(
        score_weight.reshape(
            lax.axis_size("y"), lax.axis_size("x"), cores, owned_rows
        ).transpose(1, 0, 2, 3),
        core,
        2,
        keepdims=False,
    ).reshape(chips * owned_rows, 1).astype(f32)
    code = (8 * rank_pos + relevance).astype(f32).reshape(1, groups * local)
    half = jnp.repeat(0.5 / ideal_dcg, local).reshape(1, groups * local)
    place = jnp.stack([chip, core]).astype(jnp.int32)

    slope, message = score(weight, own, other, unit, code, chips * cores)
    heard = lax.all_to_all(message, EVERY, split_axis=0, concat_axis=0, tiled=True)
    lam, term = gradient_term(heard, half, place, slope, own, other)
    lambdas = lam[0].reshape(groups, local)
    terms = lax.all_to_all(
        term.reshape(chips, owned_rows, width), CHIPS, split_axis=0, concat_axis=0, tiled=True
    )
    owned = jnp.sum(terms.astype(f32), axis=0).astype(bf16)
    across = planes * 8 // owned_rows
    owned = owned.reshape(owned_rows // 8, 8, across, width // across).transpose(0, 2, 1, 3)
    pieces = lax.all_to_all(
        owned.reshape(planes, 8, width // across), "z", split_axis=0, concat_axis=0, tiled=True
    )
    piece = jnp.sum(pieces.astype(f32), axis=0).astype(bf16)
    total = spread(piece, "z", planes)
    entries = owned_rows * width * chips * cores
    square = lax.all_to_all(
        squares(total, chips * cores), EVERY, split_axis=0, concat_axis=0, tiled=True
    )
    return scaled(total, square, owned_rows, width, entries), lambdas


def solution(mesh):
    fine = Mesh(mesh.devices.reshape(mesh.devices.shape[0], 4, 4, 2), ("z", "y", "x", "c"))
    return jax.shard_map(
        per_device,
        mesh=fine,
        in_specs=(
            P("z", CAND, None),
            P(CAND, None),
            P(),
            P("z", CAND),
            P("z", CAND),
            P("z"),
        ),
        out_specs=(P(CAND, None), P("z", CAND)),
        check_vma=False,
    )
```
